32 devices in a mesh: dp: 16 (over z, y, x), tensor: 2 (over core).
Axes of the slice: x: 2, y: 2, z: 4, core: 2. Of those that a mesh axis runs over, the one named last changes fastest.
Arguments:
- vis_rows: bfloat16 [8, 128, 2, 3200], P(None, 'dp', None, 'tensor'), may hold values from -6 to 6
- ln_gain: float32 [2, 3200], replicated, may hold values from 0.25 to 1.75
- ln_bias: float32 [2, 3200], replicated, may hold values from -3 to 3
- proj_weight: bfloat16 [3200, 2, 8192], P('dp', None, 'tensor'), may hold values from -0.078125 to 0.078125
- text_rows: bfloat16 [16, 384, 8192], P('dp', None, 'tensor'), may hold values from -8 to 8
- attn_gain: float32 [8192], replicated, may hold values from 0.25 to 1.75
- w_query: bfloat16 [8192, 4096], P('dp', 'tensor'), may hold values from -0.088388348 to 0.088388348
- key_value_weight: bfloat16 [8192, 2, 1024], P('dp', None, 'tensor'), may hold values from -0.088388348 to 0.088388348
- tile_counts: int32 [16], replicated, may hold values from 1 to 16, 128 in all
- image_offsets: int32 [16], P('dp'), may hold values from 0 to 256
Outputs:
- attn_context: bfloat16 [16, 384, 4096], P('dp', None, 'tensor')
The draws below stay inside these ranges and needn't reach their ends.
Inputs may be any that keep to these rules, and one draw needn't show every extreme that they name: tile_counts counts all 128 tiles, and its largest entry is exactly 16.
All inputs are finite; a program needn't handle non-finite values.
Results may differ from the reference program's by a relative error of at most 0.0074.
Values may be sent and summed in bfloat16 or wider, within the bound.
A program may use at most 128 MiB of HBM per device.

```python
import math
import jax
import jax.numpy as jnp
import numpy as np
from jax import lax

DV = 3200
MERGE = 2
PW = 6400
MODEL_WIDTH = 8192
QUERY_HEADS = 32
KEY_VALUE_HEADS = 8
HEAD_WIDTH = 128
TILE_DEV = 8
TILE_TOK = 8
SEQUENCE_LENGTH = 384
SAMPLES = 16
TILES = 128
ROW_TOK = 128
MAXT_TILES = 16
N_DP = 16


def draw_w_query(key, part):
    bound_value = 8.0 * MODEL_WIDTH ** (-0.5)
    sampled_values = jnp.clip(jax.random.normal(jax.random.fold_in(key, 1), (MODEL_WIDTH, QUERY_HEADS * HEAD_WIDTH), jnp.float32), -4.0, 4.0) * MODEL_WIDTH ** (-0.5)
    return jnp.clip(sampled_values, -bound_value, bound_value).astype(jnp.bfloat16)


def draw_key_value_weight(key, part):
    bound_value = 8.0 * MODEL_WIDTH ** (-0.5)
    sampled_values = jnp.clip(jax.random.normal(jax.random.fold_in(key, 2), (MODEL_WIDTH, 2, KEY_VALUE_HEADS * HEAD_WIDTH), jnp.float32), -4.0, 4.0) * MODEL_WIDTH ** (-0.5)
    return jnp.clip(sampled_values, -bound_value, bound_value).astype(jnp.bfloat16)


def draw_text_rows(key, part):
    sampled_values = jnp.clip(jax.random.normal(jax.random.fold_in(key, 3), (SAMPLES, SEQUENCE_LENGTH, MODEL_WIDTH), jnp.float32), -5.0, 5.0)
    return jnp.clip(sampled_values, -8.0, 8.0).astype(jnp.bfloat16)


def with_ends(entries, own_key, smallest, top_value):
    index_at = [jax.random.randint(jax.random.fold_in(own_key, axis), (), 0, length) for axis, length in enumerate(entries.shape)]
    widest = entries.shape.index(max(entries.shape))
    beside = index_at[:widest] + [(index_at[widest] + 1) % entries.shape[widest]] + index_at[widest + 1:]
    return entries.at[tuple(index_at)].set(smallest).at[tuple(beside)].set(top_value)


def shard_levels(key, dims, pieces, smallest, largest):
    def one(axis_at, shards_of):
        draws = jax.random.uniform(jax.random.fold_in(jax.random.fold_in(key, 6), axis_at), (shards_of,), jnp.float32, smallest / len(pieces), largest / len(pieces))
        return jnp.repeat(jnp.exp(draws), dims[axis_at] // shards_of).reshape((-1,) + (1,) * (len(dims) - axis_at - 1))

    level = one(*pieces[0])
    for cut in pieces[1:]:
        level = level * one(*cut)
    return level


def profile(number_of, total, most, lean):
    loads = [(1 << 20) // math.isqrt(rank ** lean) + 1 for rank in range(2, number_of + 1)]
    spare, given = total - most - (number_of - 1), [1] * (number_of - 1)
    while spare > 0:
        movable = [i for i in range(number_of - 1) if given[i] < most]
        pool, left = sum([loads[i] for i in movable]), spare
        for i in movable:
            extra = min(most - given[i], max(1, left * loads[i] // pool), spare)
            given[i] = given[i] + extra
            spare = spare - extra
    return np.array([most] + given)


def uneven_parts(stream_key, number_of, total, most, slope):
    if number_of == 2:
        one = jax.random.randint(stream_key, (), max(1, total - most), min(most, total - 1) + 1)
        return jnp.stack([one, total - one])
    lengths = jnp.asarray(profile(number_of, total, most, slope), jnp.int32)
    couples = (number_of - 1) // 2
    source_of, receiver = lengths[1:1 + 2 * couples:2], lengths[2:2 + 2 * couples:2]
    room = jnp.minimum(source_of - 1, most - receiver)
    moved = jax.random.randint(jax.random.fold_in(stream_key, 1), (couples,), 0, 1 << 20) % (room + 1)
    lengths = lengths.at[1:1 + 2 * couples:2].set(source_of - moved).at[2:2 + 2 * couples:2].set(receiver + moved)
    return lengths[jax.random.permutation(jax.random.fold_in(stream_key, 2), number_of)]


def normal_values(own_key, dims, scale, bound, split=(), kind=jnp.bfloat16):
    level = shard_levels(own_key, dims, split, -0.22, 0.18) if split else 1.0
    entries = jax.random.normal(own_key, dims, jnp.float32) * scale * level
    return jnp.minimum(jnp.maximum(entries, -bound), bound).astype(kind)


def setup_inputs(seed: int = 0) -> dict:
    key_of = jax.random.split(jax.random.key(seed), 11)
    return {
        "vis_rows": normal_values(key_of[0], (TILE_DEV, ROW_TOK, MERGE, DV), 1.0, 6.0, ((1, 16), (3, 2))),
        "ln_gain": jnp.clip(1.0 + 0.15 * jax.random.normal(key_of[1], (MERGE, DV), jnp.float32), 0.25, 1.75),
        "ln_bias": normal_values(key_of[2], (MERGE, DV), 0.5, 3.0, (), jnp.float32),
        "proj_weight": normal_values(key_of[3], (DV, MERGE, MODEL_WIDTH), PW ** -0.5, 0.078125, ((0, 16), (2, 2))),
        "text_rows": draw_text_rows(jax.random.fold_in(key_of[10], 71), 0),
        "attn_gain": jnp.clip(1.0 + 0.15 * jax.random.normal(key_of[5], (MODEL_WIDTH,), jnp.float32), 0.25, 1.75),
        "w_query": draw_w_query(jax.random.fold_in(key_of[10], 71), 0),
        "key_value_weight": draw_key_value_weight(jax.random.fold_in(key_of[10], 71), 0),
        "tile_counts": uneven_parts(key_of[8], SAMPLES, TILES, MAXT_TILES, 2).astype(jnp.int32),
        "image_offsets": with_ends(jax.random.randint(key_of[9], (SAMPLES,), 0, SEQUENCE_LENGTH - MAXT_TILES * TILE_TOK + 1), jax.random.fold_in(key_of[9], 1), 0, SEQUENCE_LENGTH - MAXT_TILES * TILE_TOK).astype(jnp.int32),
    }


vision_epsilon = 1e-06
decoder_epsilon = 1e-05
rope_base = 500000.0

def apply_rotary(value_rows, position_indices):
    half_width = value_rows.shape[-1] // 2
    exponents = jnp.arange(half_width, dtype=jnp.float32) * (2.0 / value_rows.shape[-1])
    frequency = rope_base ** (-exponents)
    angles = position_indices.astype(jnp.float32)[:, None] * frequency[None, :]
    cosine = jnp.cos(angles)[:, None, :]
    sine = jnp.sin(angles)[:, None, :]
    first_half = value_rows[..., :half_width]
    second_half = value_rows[..., half_width:]
    return jnp.concatenate([first_half * cosine - second_half * sine, second_half * cosine + first_half * sine], axis=-1)

def layer_norm(value_rows, gain, bias_values):
    average = lax.optimization_barrier(jnp.mean(value_rows, axis=(-2, -1), keepdims=True))
    centered = value_rows - average
    variance = lax.optimization_barrier(jnp.mean(centered * centered, axis=(-2, -1), keepdims=True))
    return centered * lax.rsqrt(variance + vision_epsilon) * gain + bias_values

def decoder_sample(sequence, w_query, key_value_weight, attn_gain):
    seq_float = sequence.astype(jnp.float32)
    mean_square = lax.optimization_barrier(jnp.mean(seq_float * seq_float, axis=-1, keepdims=True))
    normalized_sequence = (seq_float * lax.rsqrt(mean_square + decoder_epsilon) * attn_gain).astype(jnp.bfloat16)
    query_full = jnp.dot(normalized_sequence, w_query, preferred_element_type=jnp.float32)
    key_value_complete = jnp.dot(normalized_sequence, key_value_weight.reshape(MODEL_WIDTH, 2 * KEY_VALUE_HEADS * HEAD_WIDTH), preferred_element_type=jnp.float32)
    key_value_complete = key_value_complete.reshape(SEQUENCE_LENGTH, 2, KEY_VALUE_HEADS * HEAD_WIDTH)
    position_indices = jnp.arange(SEQUENCE_LENGTH, dtype=jnp.int32)
    query_group_count = QUERY_HEADS // KEY_VALUE_HEADS
    query_rows = apply_rotary(query_full.reshape(SEQUENCE_LENGTH, QUERY_HEADS, HEAD_WIDTH), position_indices).astype(jnp.bfloat16)
    query_rows = query_rows.reshape(SEQUENCE_LENGTH, KEY_VALUE_HEADS, query_group_count, HEAD_WIDTH)
    key_rows = apply_rotary(key_value_complete[:, 0].reshape(SEQUENCE_LENGTH, KEY_VALUE_HEADS, HEAD_WIDTH), position_indices).astype(jnp.bfloat16)
    value_rows = key_value_complete[:, 1].reshape(SEQUENCE_LENGTH, KEY_VALUE_HEADS, HEAD_WIDTH).astype(jnp.bfloat16)
    scores = jnp.einsum('pgjd,kgd->gjpk', query_rows.astype(jnp.float32), key_rows.astype(jnp.float32)) * HEAD_WIDTH ** (-0.5)
    causal = position_indices[:, None] >= position_indices[None, :]
    scores = jnp.where(causal[None, None], scores, -1e+30)
    row_max = lax.optimization_barrier(jnp.max(scores, axis=-1, keepdims=True))
    exponentials = jnp.exp(scores - row_max)
    weights = (exponentials / lax.optimization_barrier(jnp.sum(exponentials, axis=-1, keepdims=True))).astype(jnp.bfloat16)
    context = jnp.einsum('gjpk,kgd->pgjd', weights.astype(jnp.float32), value_rows.astype(jnp.float32))
    return context.astype(jnp.bfloat16).reshape(SEQUENCE_LENGTH, QUERY_HEADS * HEAD_WIDTH)

def reference(vis_rows, ln_gain, ln_bias, proj_weight, text_rows, attn_gain, w_query, key_value_weight, tile_counts, image_offsets):
    merged = vis_rows.reshape(TILE_DEV * ROW_TOK, MERGE, DV).astype(jnp.float32)
    normed_vis = layer_norm(merged, ln_gain, ln_bias).astype(jnp.bfloat16)
    flat_weight = jnp.transpose(proj_weight, (1, 0, 2)).reshape(MERGE * DV, MODEL_WIDTH)
    image_cols = jnp.dot(normed_vis.reshape(TILE_DEV * ROW_TOK, MERGE * DV), flat_weight, preferred_element_type=jnp.float32).astype(jnp.bfloat16)
    image_tiles = image_cols.reshape(TILE_DEV, N_DP, TILE_TOK, MODEL_WIDTH).reshape(TILES, TILE_TOK, MODEL_WIDTH)
    tile_ends = jnp.cumsum(tile_counts).astype(jnp.int32)
    tile_first = (tile_ends - tile_counts).astype(jnp.int32)
    tile_order = jnp.arange(MAXT_TILES, dtype=jnp.int32)
    image_span = MAXT_TILES * TILE_TOK

    def per_sample(inputs):
        sequence, first_tile, count, offset = inputs
        picked = jnp.clip(first_tile + tile_order, 0, TILES - 1).astype(jnp.int32)
        arrived = image_tiles[picked].reshape(image_span, MODEL_WIDTH)
        start_row = offset.astype(jnp.int32)
        current = lax.dynamic_slice_in_dim(sequence, start_row, image_span, 0)
        is_image = jnp.repeat(tile_order < count, TILE_TOK)[:, None]
        merged_rows = jnp.where(is_image, arrived, current)
        sequence = lax.dynamic_update_slice_in_dim(sequence, merged_rows, start_row, 0)
        return decoder_sample(sequence, w_query, key_value_weight, attn_gain)
    return lax.map(per_sample, (text_rows, tile_first, tile_counts, image_offsets))
```

```python
import functools
import math

import jax
import jax.numpy as jnp
from jax import lax
from jax.experimental import pallas as pl
from jax.experimental.pallas import tpu as pltpu
from jax.sharding import PartitionSpec as P

QUERY_HEADS = 32
KEY_VALUE_HEADS = 8
HEAD_WIDTH = 128


vision_epsilon = 1e-06
decoder_epsilon = 1e-05
rope_base = 500000.0

MESH = pl.DeviceIdType.MESH
NEAR = 4


def near_of(index, mid):
    return index // (2 * mid) % 2 * 2 + index % 2


def far_of(index, mid):
    return index // (4 * mid) * mid + index // 2 % mid


def join(near, far, mid):
    return (far // mid * 2 + near // 2) * (2 * mid) + far % mid * 2 + near % 2


def middle(data_count, tensor_count):
    spare = int(math.log2(data_count)) - int(math.log2(tensor_count)) - 1
    return 1 << (min(2, spare) - 1)


def here(mid):
    data_index = lax.axis_index("dp")
    return near_of(data_index, mid), far_of(data_index, mid), lax.axis_index("tensor")


def meet(mid, near=True, far=True, twin=True):
    me, my_far, tensor_index = here(mid)
    far_count = lax.axis_size("dp") // NEAR
    tensor_count = lax.axis_size("tensor")
    targets = []
    if near:
        targets += [{"dp": join((me + s) % NEAR, my_far, mid)} for s in range(1, NEAR)]
    if far:
        targets += [{"dp": join(me, (my_far + s) % far_count, mid)} for s in range(1, far_count)]
    if twin:
        targets += [{"tensor": (tensor_index + s) % tensor_count} for s in range(1, tensor_count)]
    barrier = pltpu.get_barrier_semaphore()
    for target in targets:
        pl.semaphore_signal(barrier, inc=1, device_id=target, device_id_type=MESH)
    pl.semaphore_wait(barrier, len(targets))


def remote(src_ref, dst_ref, send_sem, recv_sem, device):
    return pltpu.make_async_remote_copy(
        src_ref=src_ref,
        dst_ref=dst_ref,
        send_sem=send_sem,
        recv_sem=recv_sem,
        device_id=device,
        device_id_type=MESH,
    )


def front_kernel(mid, x_ref, gain_ref, bias_ref, pw_ref, pwg_ref, vg_ref, normed, stat_out,
                 stat_in, pw_send, pw_recv, st_send, st_recv, far_send, far_recv, near_send,
                 near_recv, twin_send, twin_recv):
    blocks, tokens, width = x_ref.shape
    far_count = vg_ref.shape[1]
    rows, wide = pwg_ref.shape[1:]
    tensor_count = lax.axis_size("tensor")
    me, my_far, tensor_index = here(mid)
    meet(mid)
    pw_copies = []
    for step in range(1, NEAR):
        target = (me + step) % NEAR
        copy = remote(
            pw_ref.at[:, pl.ds(pl.multiple_of(target * wide, wide), wide)],
            pwg_ref.at[me],
            pw_send.at[step - 1],
            pw_recv.at[step - 1],
            {"dp": join(target, my_far, mid)},
        )
        copy.start()
        pw_copies.append(copy)

    count = blocks * width
    total = jnp.zeros((tokens, 1), jnp.float32)
    for at in range(blocks):
        total = total + jnp.sum(x_ref[at].astype(jnp.float32), axis=-1, keepdims=True)
    mean = total / count
    spread = jnp.zeros((tokens, 1), jnp.float32)
    for at in range(blocks):
        centered = x_ref[at].astype(jnp.float32) - mean
        spread = spread + jnp.sum(centered * centered, axis=-1, keepdims=True)
    stat_out[0] = jnp.broadcast_to(mean, stat_out.shape[1:])
    stat_out[1] = jnp.broadcast_to(spread, stat_out.shape[1:])
    stat_copies = []
    for step in range(1, tensor_count):
        copy = remote(
            stat_out,
            stat_in.at[step - 1],
            st_send.at[step - 1],
            st_recv.at[step - 1],
            {"tensor": (tensor_index + step) % tensor_count},
        )
        copy.start()
        stat_copies.append(copy)
    for copy in stat_copies:
        copy.wait_recv()
    means, spreads = [mean], [spread]
    for step in range(1, tensor_count):
        means.append(stat_in[step - 1, 0][:, :1])
        spreads.append(stat_in[step - 1, 1][:, :1])
    average = sum(means) / tensor_count
    variance = sum(s + count * (one - average) * (one - average) for s, one in zip(spreads, means))
    scale = lax.rsqrt(variance / (count * tensor_count) + vision_epsilon)
    far_copies = []
    for at in range(blocks):
        centered = (x_ref[at].astype(jnp.float32) - average) * scale
        normed[at] = (centered * gain_ref[pl.ds(at, 1)] + bias_ref[pl.ds(at, 1)]).astype(
            normed.dtype
        )
        goal = tensor_index * blocks + at
        mine = goal == my_far
        copy = remote(
            normed.at[at],
            vg_ref.at[me, my_far],
            far_send.at[at],
            far_recv.at[my_far],
            {"dp": join(me, goal, mid)},
        )
        pl.when(jnp.logical_not(mine))(copy.start)
        far_copies.append((mine, copy))

        @pl.when(mine)
        def _():
            vg_ref[me, my_far] = normed[at]

    holder = my_far // blocks == tensor_index

    def twin_copy(ahead, step, block):
        return remote(
            vg_ref.at[block],
            vg_ref.at[block],
            twin_send.at[ahead - 1, step],
            twin_recv.at[step],
            {"tensor": (tensor_index + ahead) % tensor_count},
        )

    @pl.when(holder)
    def _():
        for step in range(1, far_count):
            source = (my_far + step) % far_count
            remote(
                normed.at[0],
                vg_ref.at[me, source],
                far_send.at[0],
                far_recv.at[source],
                {"dp": join(me, source, mid)},
            ).wait_recv()
        near_copies, twin_copies = [], []
        for step in range(1, NEAR):
            copy = remote(
                vg_ref.at[me],
                vg_ref.at[me],
                near_send.at[step - 1],
                near_recv.at[step - 1],
                {"dp": join((me + step) % NEAR, my_far, mid)},
            )
            copy.start()
            near_copies.append(copy)
        for step in range(NEAR):
            block = (me + NEAR - step) % NEAR
            if step:
                remote(
                    vg_ref.at[me],
                    vg_ref.at[block],
                    near_send.at[step - 1],
                    near_recv.at[step - 1],
                    {"dp": join(block, my_far, mid)},
                ).wait_recv()
            for ahead in range(1, tensor_count):
                copy = twin_copy(ahead, step, block)
                copy.start()
                twin_copies.append(copy)
        for copy in near_copies + twin_copies:
            copy.wait_send()

    def keep(at, carry):
        window = pl.ds(pl.multiple_of(at * 16, 16), 16)
        pwg_ref[me, window] = pw_ref[window, pl.ds(pl.multiple_of(me * wide, wide), wide)]
        return carry

    lax.fori_loop(0, rows // 16, keep, 0)

    @pl.when(jnp.logical_not(holder))
    def _():
        for step in range(NEAR):
            twin_copy(1, step, (me + NEAR - step) % NEAR).wait_recv()

    for mine, copy in far_copies:
        pl.when(jnp.logical_not(mine))(copy.wait_send)
    for copy in stat_copies:
        copy.wait_send()
    for copy in pw_copies:
        copy.wait()


def front(x, gain, bias, proj, data_count, tensor_count, mid):
    blocks, tokens, width = x.shape
    far_count = data_count // NEAR
    rows, columns = proj.shape
    vmem = pl.BlockSpec(memory_space=pltpu.VMEM)
    dma = pltpu.SemaphoreType.DMA
    return pl.pallas_call(
        functools.partial(front_kernel, mid),
        out_shape=(
            jax.ShapeDtypeStruct((NEAR, rows, columns // NEAR), proj.dtype),
            jax.ShapeDtypeStruct((NEAR, far_count, tokens, width), x.dtype),
        ),
        in_specs=[vmem] * 4,
        out_specs=(vmem, vmem),
        scratch_shapes=[
            pltpu.VMEM((blocks, tokens, width), x.dtype),
            pltpu.VMEM((2, tokens, 128), jnp.float32),
            pltpu.VMEM((tensor_count - 1, 2, tokens, 128), jnp.float32),
            dma((NEAR - 1,)),
            dma((NEAR - 1,)),
            dma((tensor_count - 1,)),
            dma((tensor_count - 1,)),
            dma((blocks,)),
            dma((far_count,)),
            dma((NEAR - 1,)),
            dma((NEAR - 1,)),
            dma((tensor_count - 1, NEAR)),
            dma((NEAR,)),
        ],
        compiler_params=pltpu.CompilerParams(
            collective_id=0, has_side_effects=True, vmem_limit_bytes=40 << 20
        ),
        cost_estimate=pl.CostEstimate(flops=0, bytes_accessed=80 << 20, transcendentals=0),
    )(x, gain, bias, proj)


def far_order(far_count):
    half = far_count // 2
    return [half] + [s for s in range(1, far_count) if s != half]


def project_kernel(mid, tile, rows, vg_ref, pw_ref, o_ref, total, leaving, held, send, recv):
    near, far_count, tokens, width = vg_ref.shape
    me, my_far, _ = here(mid)
    columns = o_ref.shape[1]

    def compute(block, dst_ref):
        def one(at, carry):
            part = pl.ds(pl.multiple_of(at * tile, tile), tile)
            term = jnp.dot(
                vg_ref[:, block].reshape(near * tokens, width),
                pw_ref[:, part],
                preferred_element_type=jnp.float32,
            )
            dst_ref[:, part] = term.astype(dst_ref.dtype)
            return carry

        lax.fori_loop(0, columns // tile, one, 0)

    meet(mid, near=False, twin=False)
    copies = []
    for step in far_order(far_count):
        target = (my_far + step) % far_count
        compute(target, leaving.at[step - 1])
        copy = remote(
            leaving.at[step - 1],
            held.at[step - 1],
            send.at[step - 1],
            recv.at[step - 1],
            {"dp": join(me, target, mid)},
        )
        copy.start()
        copies.append(copy)
    compute(my_far, total)
    for copy in copies:
        copy.wait_recv()

    def add(at, carry):
        window = pl.ds(pl.multiple_of(at * rows, rows), rows)
        value = total[window, :]
        for step in range(1, far_count):
            value = value + held[step - 1, window, :].astype(jnp.float32)
        o_ref[window, :] = value.astype(o_ref.dtype)
        return carry

    lax.fori_loop(0, o_ref.shape[0] // rows, add, 0)
    for copy in copies:
        copy.wait_send()


def project(vg, pw, mid):
    near, far_count, tokens, width = vg.shape
    columns = pw.shape[1]
    shape = (near * tokens, columns)
    dma = pltpu.SemaphoreType.DMA
    return pl.pallas_call(
        functools.partial(project_kernel, mid, math.gcd(columns, 512), 16),
        out_shape=jax.ShapeDtypeStruct(shape, vg.dtype),
        in_specs=[pl.BlockSpec(memory_space=pltpu.VMEM)] * 2,
        out_specs=pl.BlockSpec(memory_space=pltpu.VMEM),
        scratch_shapes=[
            pltpu.VMEM(shape, jnp.float32),
            pltpu.VMEM((far_count - 1,) + shape, vg.dtype),
            pltpu.VMEM((far_count - 1,) + shape, vg.dtype),
            dma((far_count - 1,)),
            dma((far_count - 1,)),
        ],
        compiler_params=pltpu.CompilerParams(
            collective_id=1, has_side_effects=True, vmem_limit_bytes=40 << 20
        ),
        cost_estimate=pl.CostEstimate(
            flops=2 * far_count * near * tokens * width * columns,
            bytes_accessed=80 << 20,
            transcendentals=0,
        ),
    )(vg, pw)


def route_kernel(mid, x_ref, o_ref, send, recv, own_sem):
    size = x_ref.shape[0]
    data_index = lax.axis_index("dp")
    me, my_far, _ = here(mid)
    own = pltpu.make_async_copy(x_ref.at[data_index], o_ref.at[me, my_far], own_sem)
    own.start()
    barrier = pltpu.get_barrier_semaphore()
    for step in range(1, size):
        pl.semaphore_signal(
            barrier,
            inc=1,
            device_id={"dp": (data_index + step) % size},
            device_id_type=MESH,
        )
    pl.semaphore_wait(barrier, size - 1)
    copies = []
    for step in range(1, size):
        target = (data_index + step) % size
        copy = remote(
            x_ref.at[target],
            o_ref.at[me, my_far],
            send.at[step - 1],
            recv.at[step - 1],
            {"dp": target},
        )
        copy.start()
        copies.append(copy)
    own.wait()
    for copy in copies:
        copy.wait()


def route(tiles, mid):
    size = tiles.shape[0]
    dma = pltpu.SemaphoreType.DMA
    return pl.pallas_call(
        functools.partial(route_kernel, mid),
        out_shape=jax.ShapeDtypeStruct((NEAR, size // NEAR) + tiles.shape[1:], tiles.dtype),
        in_specs=[pl.BlockSpec(memory_space=pltpu.VMEM)],
        out_specs=pl.BlockSpec(memory_space=pltpu.VMEM),
        scratch_shapes=[dma((size - 1,)), dma((size - 1,)), dma],
        compiler_params=pltpu.CompilerParams(
            collective_id=2, has_side_effects=True, vmem_limit_bytes=24 << 20
        ),
        cost_estimate=pl.CostEstimate(flops=0, bytes_accessed=40 << 20, transcendentals=0),
    )(tiles)


def sequence_kernel(mid, rows, spot_ref, text_ref, got_ref, gain_ref, a_ref, seq, sums, sums_in,
                    leaving, st_send, st_recv, near_send, near_recv, twin_send, twin_recv):
    tensor_count, _, seq_len, held = a_ref.shape
    near, _, wide = got_ref.shape
    model_width = text_ref.shape[1] * tensor_count
    me, my_far, tensor_index = here(mid)
    shift = held // (lax.axis_size("dp") // NEAR // tensor_count)
    meet(mid, far=False)

    def fill(at, carry):
        window = pl.ds(pl.multiple_of(at * rows, rows), rows)
        place = lax.broadcasted_iota(jnp.int32, (rows, spot_ref.shape[1]), 0) + at * rows
        chosen = jnp.where(place == spot_ref[...], 1.0, 0.0)
        image = jnp.max(chosen, axis=-1, keepdims=True) > 0.5
        chosen = chosen.astype(jnp.bfloat16)
        squares = jnp.zeros((rows, 1), jnp.float32)
        for part in range(near):
            lanes = pl.ds(part * wide, wide)
            drawn = jnp.dot(chosen, got_ref[part], preferred_element_type=jnp.float32)
            value = jnp.where(image, drawn, text_ref[window, lanes].astype(jnp.float32))
            seq[window, lanes] = value.astype(seq.dtype)
            squares = squares + jnp.sum(value * value, axis=-1, keepdims=True)
        sums[window, :] = jnp.broadcast_to(squares, (rows, sums.shape[1]))
        return carry

    lax.fori_loop(0, seq_len // rows, fill, 0)
    stat_copies = []
    for step in range(1, tensor_count):
        copy = remote(
            sums,
            sums_in.at[step - 1],
            st_send.at[step - 1],
            st_recv.at[step - 1],
            {"tensor": (tensor_index + step) % tensor_count},
        )
        copy.start()
        stat_copies.append(copy)
    for copy in stat_copies:
        copy.wait_recv()

    def norm(target, store):
        def one(at, carry):
            window = pl.ds(pl.multiple_of(at * rows, rows), rows)
            squares = sums[window, :][:, :1]
            for step in range(1, tensor_count):
                squares = squares + sums_in[step - 1, window, :][:, :1]
            scale = lax.rsqrt(squares / model_width + decoder_epsilon)
            for part in range(held // shift):
                lanes = pl.ds(pl.multiple_of(join(target, part, mid) * shift, shift), shift)
                value = seq[window, lanes].astype(jnp.float32) * scale * gain_ref[:, lanes]
                store(window, pl.ds(part * shift, shift), value.astype(jnp.bfloat16))
            return carry

        lax.fori_loop(0, seq_len // rows, one, 0)

    near_copies, twin_copies = [], []
    for step in range(1, NEAR):
        target = (me + step) % NEAR

        def leave(window, lanes, value):
            leaving[step - 1, window, lanes] = value

        norm(target, leave)
        copy = remote(
            leaving.at[step - 1],
            a_ref.at[tensor_index, me],
            near_send.at[step - 1],
            near_recv.at[step - 1],
            {"dp": join(target, my_far, mid)},
        )
        copy.start()
        near_copies.append(copy)

    def stay(window, lanes, value):
        a_ref[tensor_index, me, window, lanes] = value

    norm(me, stay)

    def twin_copy(ahead, step, owner):
        block = (me + NEAR - step) % NEAR
        return remote(
            a_ref.at[owner, block],
            a_ref.at[owner, block],
            twin_send.at[ahead - 1, step],
            twin_recv.at[ahead - 1, step],
            {"tensor": (tensor_index + ahead) % tensor_count},
        )

    for step in range(NEAR):
        if step:
            remote(
                leaving.at[step - 1],
                a_ref.at[tensor_index, (me + NEAR - step) % NEAR],
                near_send.at[step - 1],
                near_recv.at[step - 1],
                {"dp": join((me + step) % NEAR, my_far, mid)},
            ).wait_recv()
        for ahead in range(1, tensor_count):
            copy = twin_copy(ahead, step, tensor_index)
            copy.start()
            twin_copies.append(copy)
    for ahead in range(1, tensor_count):
        for step in range(NEAR):
            owner = (tensor_index + tensor_count - ahead) % tensor_count
            twin_copy(ahead, step, owner).wait_recv()
    for copy in near_copies + twin_copies + stat_copies:
        copy.wait_send()


def sequences(spots, text, got, gain, data_count, tensor_count, mid):
    seq_len, part_model = text.shape
    held = part_model // NEAR
    vmem = pl.BlockSpec(memory_space=pltpu.VMEM)
    dma = pltpu.SemaphoreType.DMA
    return pl.pallas_call(
        functools.partial(sequence_kernel, mid, math.gcd(seq_len, 32)),
        out_shape=jax.ShapeDtypeStruct((tensor_count, NEAR, seq_len, held), text.dtype),
        in_specs=[vmem] * 4,
        out_specs=vmem,
        scratch_shapes=[
            pltpu.VMEM((seq_len, part_model), text.dtype),
            pltpu.VMEM((seq_len, 128), jnp.float32),
            pltpu.VMEM((tensor_count - 1, seq_len, 128), jnp.float32),
            pltpu.VMEM((NEAR - 1, seq_len, held), text.dtype),
            dma((tensor_count - 1,)),
            dma((tensor_count - 1,)),
            dma((NEAR - 1,)),
            dma((NEAR - 1,)),
            dma((tensor_count - 1, NEAR)),
            dma((tensor_count - 1, NEAR)),
        ],
        compiler_params=pltpu.CompilerParams(
            collective_id=3, has_side_effects=True, vmem_limit_bytes=40 << 20
        ),
        cost_estimate=pl.CostEstimate(flops=0, bytes_accessed=100 << 20, transcendentals=0),
    )(spots, text, got, gain)


def product_kernel(mid, tile, rows, a_ref, w_ref, o_ref, leaving, held, send_sem, recv_sem):
    count, _, seq_len, depth = a_ref.shape
    me, my_far, _ = here(mid)
    tiles = o_ref.shape[1] // tile

    def compute(block, dst_ref, low, high):
        def one(at, carry):
            part = pl.ds(pl.multiple_of(at * tile, tile), tile)
            total = None
            for piece in range(count):
                term = jnp.dot(
                    a_ref[piece, block],
                    w_ref[pl.ds(piece * depth, depth), part],
                    preferred_element_type=jnp.float32,
                )
                total = term if total is None else total + term
            dst_ref[:, part] = total.astype(dst_ref.dtype)
            return carry

        lax.fori_loop(low, high, one, 0)

    meet(mid, far=False, twin=False)
    copies = []
    for step in range(1, NEAR + 1):
        block = (me + step) % NEAR
        dst_ref = leaving.at[step - 1] if step < NEAR else o_ref
        compute(block, dst_ref, 0, 1)
        if copies:
            copies[-1].start()
        compute(block, dst_ref, 1, tiles)
        if step < NEAR:
            copies.append(
                remote(
                    leaving.at[step - 1],
                    held.at[step - 1],
                    send_sem.at[step - 1],
                    recv_sem.at[step - 1],
                    {"dp": join(block, my_far, mid)},
                )
            )
    for copy in copies:
        copy.wait_recv()

    def add(at, carry):
        window = pl.ds(pl.multiple_of(at * rows, rows), rows)
        total = o_ref[window, :]
        for step in range(1, NEAR):
            total = total + held[step - 1, window, :].astype(jnp.float32)
        o_ref[window, :] = total
        return carry

    lax.fori_loop(0, seq_len // rows, add, 0)
    for copy in copies:
        copy.wait_send()


def product_blocks(a, weight, mid):
    count, _, seq_len, depth = a.shape
    columns = weight.shape[1]
    return pl.pallas_call(
        functools.partial(product_kernel, mid, math.gcd(columns, 512), math.gcd(seq_len, 16)),
        out_shape=jax.ShapeDtypeStruct((seq_len, columns), jnp.float32),
        in_specs=[pl.BlockSpec(memory_space=pltpu.VMEM)] * 2,
        out_specs=pl.BlockSpec(memory_space=pltpu.VMEM),
        scratch_shapes=[
            pltpu.VMEM((NEAR - 1, seq_len, columns), jnp.bfloat16),
            pltpu.VMEM((NEAR - 1, seq_len, columns), jnp.bfloat16),
            pltpu.SemaphoreType.DMA((NEAR - 1,)),
            pltpu.SemaphoreType.DMA((NEAR - 1,)),
        ],
        compiler_params=pltpu.CompilerParams(
            collective_id=4, has_side_effects=True, vmem_limit_bytes=56 << 20
        ),
        cost_estimate=pl.CostEstimate(
            flops=2 * count * NEAR * seq_len * depth * columns,
            bytes_accessed=200 << 20,
            transcendentals=0,
        ),
    )(a, weight)


def attend_kernel(group, q_ref, k_ref, v_ref, cos_ref, sin_ref, o_ref):
    cosine, sine = cos_ref[...], sin_ref[...]

    def turn(rows):
        return (rows * cosine + pltpu.roll(rows, HEAD_WIDTH // 2, 1) * sine).astype(jnp.bfloat16)

    key_rows = turn(k_ref[...])
    value_rows = v_ref[...].astype(jnp.bfloat16)
    seq_len = key_rows.shape[0]
    row_at = lax.broadcasted_iota(jnp.int32, (seq_len, seq_len), 0)
    column_at = lax.broadcasted_iota(jnp.int32, (seq_len, seq_len), 1)
    for head in range(group):
        part = pl.ds(head * HEAD_WIDTH, HEAD_WIDTH)
        query_rows = turn(q_ref[:, part])
        scores = lax.dot_general(
            query_rows, key_rows, (((1,), (1,)), ((), ())), preferred_element_type=jnp.float32
        ) * HEAD_WIDTH ** (-0.5)
        scores = jnp.where(row_at >= column_at, scores, -1e30)
        exponentials = jnp.exp(scores - jnp.max(scores, axis=-1, keepdims=True))
        weights = exponentials / jnp.sum(exponentials, axis=-1, keepdims=True)
        context = jnp.dot(
            weights.astype(jnp.bfloat16), value_rows, preferred_element_type=jnp.float32
        )
        o_ref[:, part] = context.astype(o_ref.dtype)


def attend(product, part_query):
    seq_len, columns = product.shape
    group = QUERY_HEADS // KEY_VALUE_HEADS
    local_kv = part_query // HEAD_WIDTH // group
    key_at = part_query // HEAD_WIDTH
    half_width = HEAD_WIDTH // 2
    exponents = jnp.arange(half_width, dtype=jnp.float32) * (2.0 / HEAD_WIDTH)
    frequency = rope_base ** (-exponents)
    angles = jnp.arange(seq_len, dtype=jnp.float32)[:, None] * frequency[None, :]
    cosine, sine = jnp.cos(angles), jnp.sin(angles)
    cosine = jnp.concatenate([cosine, cosine], axis=1)
    sine = jnp.concatenate([-sine, sine], axis=1)
    table = pl.BlockSpec((seq_len, HEAD_WIDTH), lambda g: (0, 0))
    return pl.pallas_call(
        functools.partial(attend_kernel, group),
        grid=(local_kv,),
        out_shape=jax.ShapeDtypeStruct((seq_len, part_query), jnp.bfloat16),
        in_specs=[
            pl.BlockSpec((seq_len, group * HEAD_WIDTH), lambda g: (0, g)),
            pl.BlockSpec((seq_len, HEAD_WIDTH), lambda g: (0, key_at + g)),
            pl.BlockSpec((seq_len, HEAD_WIDTH), lambda g: (0, key_at + local_kv + g)),
            table,
            table,
        ],
        out_specs=pl.BlockSpec((seq_len, group * HEAD_WIDTH), lambda g: (0, g)),
        compiler_params=pltpu.CompilerParams(vmem_limit_bytes=24 << 20),
    )(product, product, product, cosine, sine)


def per_device(
    vis_rows,
    ln_gain,
    ln_bias,
    proj_weight,
    text_rows,
    attn_gain,
    w_query,
    key_value_weight,
    tile_counts,
    image_offsets,
):
    data_count = lax.axis_size("dp")
    data_index = lax.axis_index("dp")
    tensor_count = lax.axis_size("tensor")
    tensor_index = lax.axis_index("tensor")
    tile_rows, tile_tok, merge_count, part_width = vis_rows.shape
    feature = proj_weight.shape[0]
    part_model = proj_weight.shape[2]
    tokens = tile_rows * tile_tok
    mid = middle(data_count, tensor_count)
    far_count = data_count // NEAR
    far_here = far_count // tensor_count
    depth = w_query.shape[0]
    groups = [[join(p, f, mid) for f in range(far_count)] for p in range(NEAR)]
    weight = jnp.concatenate([w_query, key_value_weight.reshape(depth, -1)], axis=1)
    weight = lax.all_gather(weight, "dp", axis=0, tiled=True, axis_index_groups=groups)

    tops = far_here // mid
    split = (tops, 2, mid, 2, feature)

    def arranged(rows):
        parts = rows.reshape(rows.shape[:-1] + split)
        lead = rows.ndim - 2
        order = (lead + 1, lead + 3) + tuple(range(lead)) + (lead + 2, lead + 4, lead, lead + 5)
        return parts.transpose(order).reshape((far_here,) + rows.shape[:lead] + (-1,))

    start = tensor_index * part_width
    gain = arranged(lax.dynamic_slice_in_dim(ln_gain, start, part_width, 1))
    bias = arranged(lax.dynamic_slice_in_dim(ln_bias, start, part_width, 1))
    rows_in = arranged(vis_rows.reshape(tokens, merge_count, part_width))
    proj = proj_weight.transpose(1, 0, 2).reshape(merge_count * feature, part_model)
    proj, normed = front(rows_in, gain, bias, proj, data_count, tensor_count, mid)
    image = project(normed, proj.reshape(-1, proj.shape[2]), mid)

    max_tiles = 2 * tile_rows
    tile_ends = jnp.cumsum(tile_counts)
    tile_firsts = tile_ends - tile_counts
    far_index = far_of(data_index, mid)
    sources = join(jnp.arange(NEAR, dtype=jnp.int32), far_index, mid)
    ranks = (sources[None, :] - tile_firsts[:, None]) % data_count
    taken = jnp.clip((tile_firsts[:, None] + ranks) // data_count, 0, tile_rows - 1)
    taken = taken + jnp.arange(NEAR, dtype=jnp.int32)[None, :] * tile_rows
    image = image.reshape(NEAR * tile_rows, tile_tok, image.shape[1])
    routed = image[taken].reshape(data_count, NEAR * tile_tok, image.shape[2])
    received = route(routed, mid).reshape(NEAR, data_count * tile_tok, image.shape[2])

    is_mine = jnp.arange(data_count, dtype=jnp.int32) == data_index
    my_first = jnp.sum(jnp.where(is_mine, tile_firsts, 0))
    my_count = jnp.sum(jnp.where(is_mine, tile_counts, 0))
    far_ids = jnp.arange(far_count, dtype=jnp.int32)[:, None]
    tile_ids = join(jnp.arange(NEAR, dtype=jnp.int32)[None, :], far_ids, mid).reshape(-1)
    order = (tile_ids - my_first) % data_count
    spots = image_offsets[0] + order * tile_tok
    spots = spots[:, None] + jnp.arange(tile_tok, dtype=jnp.int32)[None, :]
    spots = jnp.where((order < my_count)[:, None], spots, -1).reshape(1, -1)
    gain = lax.dynamic_slice_in_dim(attn_gain, tensor_index * part_model, part_model, 0)
    sequence = sequences(
        spots, text_rows[0], received, gain[None, :], data_count, tensor_count, mid
    )
    product = product_blocks(sequence, weight, mid)
    context = attend(product, w_query.shape[1])
    return context[None]


def solution(mesh):
    in_specs = (
        P(None, "dp", None, "tensor"),
        P(),
        P(),
        P("dp", None, "tensor"),
        P("dp", None, "tensor"),
        P(),
        P("dp", "tensor"),
        P("dp", None, "tensor"),
        P(),
        P("dp"),
    )
    out_specs = P("dp", None, "tensor")
    return jax.shard_map(
        per_device, mesh=mesh, in_specs=in_specs, out_specs=out_specs, check_vma=False
    )
```

```python
import functools
import math

import jax
import jax.numpy as jnp
from jax import lax
from jax.experimental import pallas as pl
from jax.experimental.pallas import tpu as pltpu
from jax.sharding import PartitionSpec as P

QUERY_HEADS = 32
KEY_VALUE_HEADS = 8
HEAD_WIDTH = 128


vision_epsilon = 1e-06
decoder_epsilon = 1e-05
rope_base = 500000.0

MESH = pl.DeviceIdType.MESH
NEAR = 4


def near_of(index, mid):
    return index // (2 * mid) % 2 * 2 + index % 2


def far_of(index, mid):
    return index // (4 * mid) * mid + index // 2 % mid


def join(near, far, mid):
    return (far // mid * 2 + near // 2) * (2 * mid) + far % mid * 2 + near % 2


def middle(data_count, tensor_count):
    spare = int(math.log2(data_count)) - int(math.log2(tensor_count)) - 1
    return 1 << (min(2, spare) - 1)


def here(mid):
    data_index = lax.axis_index("dp")
    return near_of(data_index, mid), far_of(data_index, mid), lax.axis_index("tensor")


def meet(mid, near=True, far=True, twin=True):
    me, my_far, tensor_index = here(mid)
    far_count = lax.axis_size("dp") // NEAR
    tensor_count = lax.axis_size("tensor")
    targets = []
    if near:
        targets += [{"dp": join((me + s) % NEAR, my_far, mid)} for s in range(1, NEAR)]
    if far:
        targets += [{"dp": join(me, (my_far + s) % far_count, mid)} for s in range(1, far_count)]
    if twin:
        targets += [{"tensor": (tensor_index + s) % tensor_count} for s in range(1, tensor_count)]
    barrier = pltpu.get_barrier_semaphore()
    for target in targets:
        pl.semaphore_signal(barrier, inc=1, device_id=target, device_id_type=MESH)
    pl.semaphore_wait(barrier, len(targets))


def remote(src_ref, dst_ref, send_sem, recv_sem, device):
    return pltpu.make_async_remote_copy(
        src_ref=src_ref,
        dst_ref=dst_ref,
        send_sem=send_sem,
        recv_sem=recv_sem,
        device_id=device,
        device_id_type=MESH,
    )


def flip(index, bits):
    bit = 1
    while bit <= bits:
        if bits & bit:
            index = index + bit - 2 * bit * (index // bit % 2)
        bit *= 2
    return index


def gather_items(far_count):
    items, masks, bit = [], [0], far_count // 2
    while bit:
        items += [(bit, mask) for mask in masks]
        masks = masks + [mask | bit for mask in masks]
        bit //= 2
    return items


def gather_plan(far_count, chunks):
    third = chunks // 3
    high = far_count // 2
    items = gather_items(far_count)
    plan = {"front": [], "sequence": [], "product": []}
    have = {chunk: {0} for chunk in range(chunks)}
    for name, first, others in (
        ("front", range(third), range(2 * third)),
        ("sequence", range(third, 2 * third), range(2 * third, chunks)),
    ):
        held = {chunk: set(masks) for chunk, masks in have.items()}
        done = [job for jobs in plan.values() for job in jobs]
        for chunk in range(chunks):
            for bit, mask in items:
                wanted = (chunk in first) if bit == high else (chunk in others)
                if mask:
                    wanted = name == "sequence" and chunk < third and mask in held[chunk]
                if wanted and (bit, mask, chunk) not in done:
                    plan[name].append((bit, mask, chunk))
                    have[chunk].add(bit | mask)
    done = plan["front"] + plan["sequence"]
    for chunk in range(chunks):
        plan["product"] += [
            (bit, mask, chunk) for bit, mask in items if (bit, mask, chunk) not in done
        ]
    return plan, have


def chunk_at(chunk, tile, refs, lead):
    start = chunk * tile
    for ref in refs:
        width = ref.shape[-1]
        if start < width:
            part = pl.ds(start, tile)
            return ref.at[:, part] if lead is None else ref.at[lead, :, part]
        start -= width


def weight_copies(mid, tile, jobs, own_refs, got_refs, send, recv):
    me, my_far, _ = here(mid)
    copies = []
    for at, (bit, mask, chunk) in enumerate(jobs):
        block = flip(my_far, mask)
        source = chunk_at(chunk, tile, got_refs, block) if mask else chunk_at(
            chunk, tile, own_refs, None
        )
        copies.append(
            remote(
                source,
                chunk_at(chunk, tile, got_refs, block),
                send.at[at],
                recv.at[at],
                {"dp": join(me, flip(my_far, bit), mid)},
            )
        )
    return copies


class Halving:
    def __init__(self, bits, index, device, rows, out_ref, in_ref, acc_ref, own_ref, send, recv):
        self.bits, self.index, self.device, self.rows = bits, index, device, rows
        self.out_ref, self.in_ref, self.acc_ref, self.own_ref = out_ref, in_ref, acc_ref, own_ref
        self.send, self.recv = send, recv
        size = 1 << len(bits)
        self.stage_of = {
            mask: min(at for at, bit in enumerate(bits) if mask & bit) for mask in range(1, size)
        }
        later = [mask for mask in range(1, size) if self.stage_of[mask]]
        self.slot = {mask: at for at, mask in enumerate(later)}
        self.copies = []

    def masks(self, stage):
        return [mask for mask, at in self.stage_of.items() if at == stage]

    def start(self, stage):
        bit = self.bits[stage]
        for mask in self.masks(stage):
            copy = remote(
                self.out_ref.at[mask - 1],
                self.in_ref.at[mask - 1],
                self.send.at[mask - 1],
                self.recv.at[mask - 1],
                self.device(flip(self.index, bit)),
            )
            copy.start()
            self.copies.append((stage, copy))

    def receive(self, stage):
        for at, copy in self.copies:
            if at == stage:
                copy.wait_recv()
        rows, bit = self.rows, self.bits[stage]
        last = stage + 1 == len(self.bits)

        def add(at, carry):
            window = pl.ds(pl.multiple_of(at * rows, rows), rows)
            for mask in self.masks(stage):
                value = self.in_ref[mask - 1, window, :].astype(jnp.float32)
                rest = mask - bit
                if not rest:
                    self.own_ref[window, :] = self.own_ref[window, :] + value
                else:
                    value = self.acc_ref[self.slot[rest], window, :] + value
                    if self.stage_of[rest] == stage + 1:
                        self.out_ref[rest - 1, window, :] = value.astype(self.out_ref.dtype)
                    else:
                        self.acc_ref[self.slot[rest], window, :] = value
            return carry

        lax.fori_loop(0, self.own_ref.shape[0] // rows, add, 0)
        if not last:
            self.start(stage + 1)

    def finish(self):
        for _, copy in self.copies:
            copy.wait_send()


def front_kernel(mid, tile, jobs, x_ref, gain_ref, bias_ref, pw_ref, wq_ref, wkv_ref, pwg_ref,
                 vg_ref, gq_ref, gkv_ref, normed, stat_out, stat_in, pw_send, pw_recv, st_send,
                 st_recv, far_send, far_recv, near_send, near_recv, twin_send, twin_recv, w_send,
                 w_recv):
    blocks, tokens, width = x_ref.shape
    far_count = vg_ref.shape[1]
    rows, wide = pwg_ref.shape[1:]
    tensor_count = lax.axis_size("tensor")
    me, my_far, tensor_index = here(mid)
    meet(mid)
    pw_copies = []
    for step in range(1, NEAR):
        target = (me + step) % NEAR
        copy = remote(
            pw_ref.at[:, pl.ds(pl.multiple_of(target * wide, wide), wide)],
            pwg_ref.at[me],
            pw_send.at[step - 1],
            pw_recv.at[step - 1],
            {"dp": join(target, my_far, mid)},
        )
        copy.start()
        pw_copies.append(copy)
    w_copies = weight_copies(
        mid, tile, jobs, (wq_ref, wkv_ref), (gq_ref, gkv_ref), w_send, w_recv
    )
    early = len(w_copies) // 3
    for copy in w_copies[:early]:
        copy.start()

    count = blocks * width
    total = jnp.zeros((tokens, 1), jnp.float32)
    for at in range(blocks):
        total = total + jnp.sum(x_ref[at].astype(jnp.float32), axis=-1, keepdims=True)
    mean = total / count
    spread = jnp.zeros((tokens, 1), jnp.float32)
    for at in range(blocks):
        centered = x_ref[at].astype(jnp.float32) - mean
        spread = spread + jnp.sum(centered * centered, axis=-1, keepdims=True)
    stat_out[0] = jnp.broadcast_to(mean, stat_out.shape[1:])
    stat_out[1] = jnp.broadcast_to(spread, stat_out.shape[1:])
    stat_copies = []
    for step in range(1, tensor_count):
        copy = remote(
            stat_out,
            stat_in.at[step - 1],
            st_send.at[step - 1],
            st_recv.at[step - 1],
            {"tensor": (tensor_index + step) % tensor_count},
        )
        copy.start()
        stat_copies.append(copy)
    for copy in stat_copies:
        copy.wait_recv()
    means, spreads = [mean], [spread]
    for step in range(1, tensor_count):
        means.append(stat_in[step - 1, 0][:, :1])
        spreads.append(stat_in[step - 1, 1][:, :1])
    average = sum(means) / tensor_count
    variance = sum(s + count * (one - average) * (one - average) for s, one in zip(spreads, means))
    scale = lax.rsqrt(variance / (count * tensor_count) + vision_epsilon)
    far_copies = []
    for at in range(blocks):
        centered = (x_ref[at].astype(jnp.float32) - average) * scale
        normed[at] = (centered * gain_ref[pl.ds(at, 1)] + bias_ref[pl.ds(at, 1)]).astype(
            normed.dtype
        )
        goal = tensor_index * blocks + at
        mine = goal == my_far
        copy = remote(
            normed.at[at],
            vg_ref.at[me, my_far],
            far_send.at[at],
            far_recv.at[my_far],
            {"dp": join(me, goal, mid)},
        )
        pl.when(jnp.logical_not(mine))(copy.start)
        far_copies.append((mine, copy))

        @pl.when(mine)
        def _():
            vg_ref[me, my_far] = normed[at]

    for copy in w_copies[early:]:
        copy.start()
    holder = my_far // blocks == tensor_index

    def twin_copy(ahead, step, block):
        return remote(
            vg_ref.at[block],
            vg_ref.at[block],
            twin_send.at[ahead - 1, step],
            twin_recv.at[step],
            {"tensor": (tensor_index + ahead) % tensor_count},
        )

    @pl.when(holder)
    def _():
        for step in range(1, far_count):
            source = (my_far + step) % far_count
            remote(
                normed.at[0],
                vg_ref.at[me, source],
                far_send.at[0],
                far_recv.at[source],
                {"dp": join(me, source, mid)},
            ).wait_recv()
        near_copies, twin_copies = [], []
        for step in range(1, NEAR):
            copy = remote(
                vg_ref.at[me],
                vg_ref.at[me],
                near_send.at[step - 1],
                near_recv.at[step - 1],
                {"dp": join((me + step) % NEAR, my_far, mid)},
            )
            copy.start()
            near_copies.append(copy)
        for step in range(NEAR):
            block = (me + NEAR - step) % NEAR
            if step:
                remote(
                    vg_ref.at[me],
                    vg_ref.at[block],
                    near_send.at[step - 1],
                    near_recv.at[step - 1],
                    {"dp": join(block, my_far, mid)},
                ).wait_recv()
            for ahead in range(1, tensor_count):
                copy = twin_copy(ahead, step, block)
                copy.start()
                twin_copies.append(copy)
        for copy in near_copies + twin_copies:
            copy.wait_send()

    def keep(at, carry):
        window = pl.ds(pl.multiple_of(at * 16, 16), 16)
        pwg_ref[me, window] = pw_ref[window, pl.ds(pl.multiple_of(me * wide, wide), wide)]
        return carry

    lax.fori_loop(0, rows // 16, keep, 0)

    @pl.when(jnp.logical_not(holder))
    def _():
        for step in range(NEAR):
            twin_copy(1, step, (me + NEAR - step) % NEAR).wait_recv()

    for mine, copy in far_copies:
        pl.when(jnp.logical_not(mine))(copy.wait_send)
    for copy in stat_copies:
        copy.wait_send()
    for copy in pw_copies + w_copies:
        copy.wait()


def front(x, gain, bias, proj, w_query, w_kv, tile, jobs, data_count, tensor_count, mid):
    blocks, tokens, width = x.shape
    far_count = data_count // NEAR
    rows, columns = proj.shape
    vmem = pl.BlockSpec(memory_space=pltpu.VMEM)
    anywhere = pl.BlockSpec(memory_space=pl.ANY)
    dma = pltpu.SemaphoreType.DMA
    return pl.pallas_call(
        functools.partial(front_kernel, mid, tile, jobs),
        out_shape=(
            jax.ShapeDtypeStruct((NEAR, rows, columns // NEAR), proj.dtype),
            jax.ShapeDtypeStruct((NEAR, far_count, tokens, width), x.dtype),
            jax.ShapeDtypeStruct((far_count,) + w_query.shape, w_query.dtype),
            jax.ShapeDtypeStruct((far_count,) + w_kv.shape, w_kv.dtype),
        ),
        in_specs=[vmem] * 4 + [anywhere] * 2,
        out_specs=(vmem, vmem, anywhere, anywhere),
        scratch_shapes=[
            pltpu.VMEM((blocks, tokens, width), x.dtype),
            pltpu.VMEM((2, tokens, 128), jnp.float32),
            pltpu.VMEM((tensor_count - 1, 2, tokens, 128), jnp.float32),
            dma((NEAR - 1,)),
            dma((NEAR - 1,)),
            dma((tensor_count - 1,)),
            dma((tensor_count - 1,)),
            dma((blocks,)),
            dma((far_count,)),
            dma((NEAR - 1,)),
            dma((NEAR - 1,)),
            dma((tensor_count - 1, NEAR)),
            dma((NEAR,)),
            dma((len(jobs),)),
            dma((len(jobs),)),
        ],
        compiler_params=pltpu.CompilerParams(
            collective_id=0, has_side_effects=True, vmem_limit_bytes=40 << 20
        ),
        cost_estimate=pl.CostEstimate(flops=0, bytes_accessed=80 << 20, transcendentals=0),
    )(x, gain, bias, proj, w_query, w_kv)


def project_kernel(mid, tile, vg_ref, pw_ref, o_ref, own, acc, out, held, send, recv):
    near, far_count, tokens, width = vg_ref.shape
    me, my_far, _ = here(mid)
    chunks = own.shape[0]
    bits = []
    while 1 << len(bits) < far_count:
        bits.append(1 << len(bits))

    def compute(mask, chunk, dst_ref):
        term = jnp.dot(
            vg_ref[:, flip(my_far, mask)].reshape(near * tokens, width),
            pw_ref[:, pl.ds(chunk * tile, tile)],
            preferred_element_type=jnp.float32,
        )
        dst_ref[...] = term.astype(dst_ref.dtype)

    meet(mid, near=False, twin=False)
    sums = []
    for chunk in range(chunks):
        one = Halving(
            bits, my_far, lambda far: {"dp": join(me, far, mid)}, 32, out.at[chunk],
            held.at[chunk], acc.at[chunk], own.at[chunk], send.at[chunk], recv.at[chunk],
        )
        for mask in one.masks(0):
            compute(mask, chunk, out.at[chunk, mask - 1])
        one.start(0)
        sums.append(one)
    for chunk, one in enumerate(sums):
        for mask, slot in one.slot.items():
            compute(mask, chunk, acc.at[chunk, slot])
        compute(0, chunk, own.at[chunk])
    for stage in range(len(bits)):
        for one in sums:
            one.receive(stage)
    for chunk, one in enumerate(sums):
        o_ref[:, pl.ds(chunk * tile, tile)] = own[chunk].astype(o_ref.dtype)
        one.finish()


def project(vg, pw, mid):
    near, far_count, tokens, width = vg.shape
    columns = pw.shape[1]
    tile = math.gcd(columns, 512)
    chunks, rows = columns // tile, near * tokens
    dma = pltpu.SemaphoreType.DMA
    return pl.pallas_call(
        functools.partial(project_kernel, mid, tile),
        out_shape=jax.ShapeDtypeStruct((rows, columns), vg.dtype),
        in_specs=[pl.BlockSpec(memory_space=pltpu.VMEM)] * 2,
        out_specs=pl.BlockSpec(memory_space=pltpu.VMEM),
        scratch_shapes=[
            pltpu.VMEM((chunks, rows, tile), jnp.float32),
            pltpu.VMEM((chunks, far_count // 2 - 1, rows, tile), jnp.float32),
            pltpu.VMEM((chunks, far_count - 1, rows, tile), vg.dtype),
            pltpu.VMEM((chunks, far_count - 1, rows, tile), vg.dtype),
            dma((chunks, far_count - 1)),
            dma((chunks, far_count - 1)),
        ],
        compiler_params=pltpu.CompilerParams(
            collective_id=1, has_side_effects=True, vmem_limit_bytes=40 << 20
        ),
        cost_estimate=pl.CostEstimate(
            flops=2 * far_count * near * tokens * width * columns,
            bytes_accessed=80 << 20,
            transcendentals=0,
        ),
    )(vg, pw)


def route_kernel(mid, x_ref, o_ref, send, recv, own_sem):
    size = x_ref.shape[0]
    data_index = lax.axis_index("dp")
    me, my_far, _ = here(mid)
    own = pltpu.make_async_copy(x_ref.at[data_index], o_ref.at[me, my_far], own_sem)
    own.start()
    barrier = pltpu.get_barrier_semaphore()
    for step in range(1, size):
        pl.semaphore_signal(
            barrier,
            inc=1,
            device_id={"dp": (data_index + step) % size},
            device_id_type=MESH,
        )
    pl.semaphore_wait(barrier, size - 1)
    copies = []
    for step in range(1, size):
        target = (data_index + step) % size
        copy = remote(
            x_ref.at[target],
            o_ref.at[me, my_far],
            send.at[step - 1],
            recv.at[step - 1],
            {"dp": target},
        )
        copy.start()
        copies.append(copy)
    own.wait()
    for copy in copies:
        copy.wait()


def route(tiles, mid):
    size = tiles.shape[0]
    dma = pltpu.SemaphoreType.DMA
    return pl.pallas_call(
        functools.partial(route_kernel, mid),
        out_shape=jax.ShapeDtypeStruct((NEAR, size // NEAR) + tiles.shape[1:], tiles.dtype),
        in_specs=[pl.BlockSpec(memory_space=pltpu.VMEM)],
        out_specs=pl.BlockSpec(memory_space=pltpu.VMEM),
        scratch_shapes=[dma((size - 1,)), dma((size - 1,)), dma],
        compiler_params=pltpu.CompilerParams(
            collective_id=2, has_side_effects=True, vmem_limit_bytes=24 << 20
        ),
        cost_estimate=pl.CostEstimate(flops=0, bytes_accessed=40 << 20, transcendentals=0),
    )(tiles)


def sequence_kernel(mid, rows, tile, jobs, spot_ref, text_ref, got_ref, gain_ref, wq_ref,
                    wkv_ref, gq_in, gkv_in, a_ref, gq_ref, gkv_ref, seq, sums, sums_in, leaving,
                    st_send, st_recv, near_send, near_recv, twin_send, twin_recv, w_send, w_recv):
    _, seq_len, depth = a_ref.shape
    near, _, wide = got_ref.shape
    tensor_count = lax.axis_size("tensor")
    held = depth // tensor_count
    model_width = text_ref.shape[1] * tensor_count
    me, my_far, tensor_index = here(mid)
    shift = held // (lax.axis_size("dp") // NEAR // tensor_count)
    meet(mid)
    w_copies = weight_copies(
        mid, tile, jobs, (wq_ref, wkv_ref), (gq_ref, gkv_ref), w_send, w_recv
    )
    for copy in w_copies:
        copy.start()

    def fill(at, carry):
        window = pl.ds(pl.multiple_of(at * rows, rows), rows)
        place = lax.broadcasted_iota(jnp.int32, (rows, spot_ref.shape[1]), 0) + at * rows
        chosen = jnp.where(place == spot_ref[...], 1.0, 0.0)
        image = jnp.max(chosen, axis=-1, keepdims=True) > 0.5
        chosen = chosen.astype(jnp.bfloat16)
        squares = jnp.zeros((rows, 1), jnp.float32)
        for part in range(near):
            lanes = pl.ds(part * wide, wide)
            drawn = jnp.dot(chosen, got_ref[part], preferred_element_type=jnp.float32)
            value = jnp.where(image, drawn, text_ref[window, lanes].astype(jnp.float32))
            seq[window, lanes] = value.astype(seq.dtype)
            squares = squares + jnp.sum(value * value, axis=-1, keepdims=True)
        sums[window, :] = jnp.broadcast_to(squares, (rows, sums.shape[1]))
        return carry

    lax.fori_loop(0, seq_len // rows, fill, 0)
    stat_copies = []
    for step in range(1, tensor_count):
        copy = remote(
            sums,
            sums_in.at[step - 1],
            st_send.at[step - 1],
            st_recv.at[step - 1],
            {"tensor": (tensor_index + step) % tensor_count},
        )
        copy.start()
        stat_copies.append(copy)
    for copy in stat_copies:
        copy.wait_recv()

    def norm(target, store):
        def one(at, carry):
            window = pl.ds(pl.multiple_of(at * rows, rows), rows)
            squares = sums[window, :][:, :1]
            for step in range(1, tensor_count):
                squares = squares + sums_in[step - 1, window, :][:, :1]
            scale = lax.rsqrt(squares / model_width + decoder_epsilon)
            for part in range(held // shift):
                lanes = pl.ds(pl.multiple_of(join(target, part, mid) * shift, shift), shift)
                value = seq[window, lanes].astype(jnp.float32) * scale * gain_ref[:, lanes]
                store(window, part * shift, value.astype(jnp.bfloat16))
            return carry

        lax.fori_loop(0, seq_len // rows, one, 0)

    def lanes_of(owner):
        return pl.ds(pl.multiple_of(owner * held, held), held)

    near_copies, twin_copies = [], []
    for step in range(1, NEAR):
        target = flip(me, step)

        def leave(window, start, value):
            leaving[step - 1, window, pl.ds(start, shift)] = value

        norm(target, leave)
        copy = remote(
            leaving.at[step - 1],
            a_ref.at[me, :, lanes_of(tensor_index)],
            near_send.at[step - 1],
            near_recv.at[step - 1],
            {"dp": join(target, my_far, mid)},
        )
        copy.start()
        near_copies.append(copy)

    def stay(window, start, value):
        lanes = pl.ds(pl.multiple_of(tensor_index * held + start, shift), shift)
        a_ref[me, window, lanes] = value

    norm(me, stay)

    def twin_copy(ahead, step, owner):
        block = flip(me, step)
        return remote(
            a_ref.at[block, :, lanes_of(owner)],
            a_ref.at[block, :, lanes_of(owner)],
            twin_send.at[ahead - 1, step],
            twin_recv.at[ahead - 1, step],
            {"tensor": (tensor_index + ahead) % tensor_count},
        )

    for step in range(NEAR):
        if step:
            near_copies[step - 1].wait_recv()
        for ahead in range(1, tensor_count):
            copy = twin_copy(ahead, step, tensor_index)
            copy.start()
            twin_copies.append(copy)
    for ahead in range(1, tensor_count):
        for step in range(NEAR):
            owner = (tensor_index + tensor_count - ahead) % tensor_count
            twin_copy(ahead, step, owner).wait_recv()
    for copy in near_copies + twin_copies + stat_copies:
        copy.wait_send()
    for copy in w_copies:
        copy.wait()


def sequences(spots, text, got, gain, weights, gathered, tile, jobs, tensor_count, mid):
    seq_len, part_model = text.shape
    held = part_model // NEAR
    vmem = pl.BlockSpec(memory_space=pltpu.VMEM)
    anywhere = pl.BlockSpec(memory_space=pl.ANY)
    dma = pltpu.SemaphoreType.DMA
    return pl.pallas_call(
        functools.partial(sequence_kernel, mid, math.gcd(seq_len, 32), tile, jobs),
        out_shape=(jax.ShapeDtypeStruct((NEAR, seq_len, held * tensor_count), text.dtype),)
        + tuple(jax.ShapeDtypeStruct(one.shape, one.dtype) for one in gathered),
        in_specs=[vmem] * 4 + [anywhere] * 4,
        out_specs=(vmem, anywhere, anywhere),
        input_output_aliases={6: 1, 7: 2},
        scratch_shapes=[
            pltpu.VMEM((seq_len, part_model), text.dtype),
            pltpu.VMEM((seq_len, 128), jnp.float32),
            pltpu.VMEM((tensor_count - 1, seq_len, 128), jnp.float32),
            pltpu.VMEM((NEAR - 1, seq_len, held), text.dtype),
            dma((tensor_count - 1,)),
            dma((tensor_count - 1,)),
            dma((NEAR - 1,)),
            dma((NEAR - 1,)),
            dma((tensor_count - 1, NEAR)),
            dma((tensor_count - 1, NEAR)),
            dma((len(jobs),)),
            dma((len(jobs),)),
        ],
        compiler_params=pltpu.CompilerParams(
            collective_id=3, has_side_effects=True, vmem_limit_bytes=40 << 20
        ),
        cost_estimate=pl.CostEstimate(flops=0, bytes_accessed=100 << 20, transcendentals=0),
    )(spots, text, got, gain, *weights, *gathered)


def product_kernel(mid, tile, jobs, have, a_ref, wq_ref, wkv_ref, gq_ref, gkv_ref, o_ref, w, acc,
                   out, held, send, recv, w_send, w_recv, load_sem):
    _, seq_len, _ = a_ref.shape
    depth = wq_ref.shape[0]
    far_count = gq_ref.shape[0]
    me, my_far, _ = here(mid)
    chunks = len(have)
    own_refs, got_refs = (wq_ref, wkv_ref), (gq_ref, gkv_ref)

    def place(mask, chunk):
        rows = pl.ds(pl.multiple_of(flip(my_far, mask) * depth, depth), depth)
        return w.at[rows, pl.ds(chunk * tile, tile)]

    def local(mask, chunk):
        if mask:
            return chunk_at(chunk, tile, got_refs, flip(my_far, mask))
        return chunk_at(chunk, tile, own_refs, None)

    loads = {}
    for chunk in range(chunks):
        for mask in sorted(have[chunk]):
            loads[mask, chunk] = pltpu.make_async_copy(
                local(mask, chunk), place(mask, chunk), load_sem.at[chunk, mask]
            )
            loads[mask, chunk].start()

    meet(mid, twin=False)
    arriving, waiting = {}, {chunk: [] for chunk in range(chunks)}
    for at, (bit, mask, chunk) in enumerate(jobs):
        kept = mask in have[chunk]
        copy = remote(
            local(mask, chunk) if kept else place(mask, chunk),
            place(mask, chunk),
            w_send.at[at],
            w_recv.at[at],
            {"dp": join(me, flip(my_far, bit), mid)},
        )
        arriving[bit | mask, chunk] = copy
        if kept:
            copy.start()
        else:
            waiting[chunk].append((mask, copy))
    seen = set()

    def ensure(mask, chunk):
        if (mask, chunk) not in seen:
            seen.add((mask, chunk))
            if (mask, chunk) in loads:
                loads[mask, chunk].wait()
            else:
                arriving[mask, chunk].wait_recv()

    def forward(chunk):
        for mask, copy in waiting.pop(chunk, ()):
            ensure(mask, chunk)
            copy.start()

    sums = []

    def compute(chunk):
        forward(chunk)
        for mask in range(far_count):
            ensure(mask, chunk)
        part = pl.ds(chunk * tile, tile)
        bits = (1, 2) if chunk % 2 else (2, 1)
        one = Halving(
            bits, me, lambda near: {"dp": join(near, my_far, mid)}, math.gcd(seq_len, 32),
            out.at[chunk], held.at[chunk], acc.at[chunk], o_ref.at[:, part], send.at[chunk],
            recv.at[chunk],
        )

        def fill(mask, dst_ref):
            term = jnp.dot(
                a_ref[flip(me, mask)], w[:, part], preferred_element_type=jnp.float32
            )
            dst_ref[...] = term.astype(dst_ref.dtype)

        for mask in one.masks(0):
            fill(mask, out.at[chunk, mask - 1])
        one.start(0)
        for mask, slot in one.slot.items():
            fill(mask, acc.at[chunk, slot])
        fill(0, o_ref.at[:, part])
        sums.append(one)

    done = {0: 0, 1: 0}

    def reduce(stage, upto):
        for one in sums[done[stage] : upto]:
            one.receive(stage)
        done[stage] = max(done[stage], upto)

    third = chunks // 3
    for chunk in range(2 * third):
        compute(chunk)
    reduce(0, third)
    for chunk in range(2 * third, chunks):
        forward(chunk)
        reduce(0, 2 * third)
        if chunk > 2 * third:
            reduce(1, 2 * third)
        compute(chunk)
    reduce(0, chunks)
    reduce(1, chunks)
    for one in sums:
        one.finish()
    for copy in arriving.values():
        copy.wait_send()


def product_blocks(a, weights, gathered, tile, jobs, have, mid):
    _, seq_len, depth = a.shape
    columns = sum(one.shape[1] for one in weights)
    chunks = columns // tile
    vmem = pl.BlockSpec(memory_space=pltpu.VMEM)
    anywhere = pl.BlockSpec(memory_space=pl.ANY)
    far_count = gathered[0].shape[0]
    dma = pltpu.SemaphoreType.DMA
    return pl.pallas_call(
        functools.partial(product_kernel, mid, tile, jobs, have),
        out_shape=jax.ShapeDtypeStruct((seq_len, columns), jnp.float32),
        in_specs=[vmem] + [anywhere] * 4,
        out_specs=vmem,
        scratch_shapes=[
            pltpu.VMEM((depth, columns), jnp.bfloat16),
            pltpu.VMEM((chunks, NEAR // 2 - 1, seq_len, tile), jnp.float32),
            pltpu.VMEM((chunks, NEAR - 1, seq_len, tile), jnp.bfloat16),
            pltpu.VMEM((chunks, NEAR - 1, seq_len, tile), jnp.bfloat16),
            dma((chunks, NEAR - 1)),
            dma((chunks, NEAR - 1)),
            dma((len(jobs),)),
            dma((len(jobs),)),
            dma((chunks, far_count)),
        ],
        compiler_params=pltpu.CompilerParams(
            collective_id=4, has_side_effects=True, vmem_limit_bytes=56 << 20
        ),
        cost_estimate=pl.CostEstimate(
            flops=2 * NEAR * seq_len * depth * columns,
            bytes_accessed=200 << 20,
            transcendentals=0,
        ),
    )(a, *weights, *gathered)


def attend_kernel(group, q_ref, k_ref, v_ref, cos_ref, sin_ref, o_ref):
    cosine, sine = cos_ref[...], sin_ref[...]

    def turn(rows):
        return (rows * cosine + pltpu.roll(rows, HEAD_WIDTH // 2, 1) * sine).astype(jnp.bfloat16)

    key_rows = turn(k_ref[...])
    value_rows = v_ref[...].astype(jnp.bfloat16)
    seq_len = key_rows.shape[0]
    row_at = lax.broadcasted_iota(jnp.int32, (seq_len, seq_len), 0)
    column_at = lax.broadcasted_iota(jnp.int32, (seq_len, seq_len), 1)
    for head in range(group):
        part = pl.ds(head * HEAD_WIDTH, HEAD_WIDTH)
        query_rows = turn(q_ref[:, part])
        scores = lax.dot_general(
            query_rows, key_rows, (((1,), (1,)), ((), ())), preferred_element_type=jnp.float32
        ) * HEAD_WIDTH ** (-0.5)
        scores = jnp.where(row_at >= column_at, scores, -1e30)
        exponentials = jnp.exp(scores - jnp.max(scores, axis=-1, keepdims=True))
        weights = exponentials / jnp.sum(exponentials, axis=-1, keepdims=True)
        context = jnp.dot(
            weights.astype(jnp.bfloat16), value_rows, preferred_element_type=jnp.float32
        )
        o_ref[:, part] = context.astype(o_ref.dtype)


def attend(product, part_query):
    seq_len, columns = product.shape
    group = QUERY_HEADS // KEY_VALUE_HEADS
    local_kv = part_query // HEAD_WIDTH // group
    key_at = part_query // HEAD_WIDTH
    half_width = HEAD_WIDTH // 2
    exponents = jnp.arange(half_width, dtype=jnp.float32) * (2.0 / HEAD_WIDTH)
    frequency = rope_base ** (-exponents)
    angles = jnp.arange(seq_len, dtype=jnp.float32)[:, None] * frequency[None, :]
    cosine, sine = jnp.cos(angles), jnp.sin(angles)
    cosine = jnp.concatenate([cosine, cosine], axis=1)
    sine = jnp.concatenate([-sine, sine], axis=1)
    table = pl.BlockSpec((seq_len, HEAD_WIDTH), lambda g: (0, 0))
    return pl.pallas_call(
        functools.partial(attend_kernel, group),
        grid=(local_kv,),
        out_shape=jax.ShapeDtypeStruct((seq_len, part_query), jnp.bfloat16),
        in_specs=[
            pl.BlockSpec((seq_len, group * HEAD_WIDTH), lambda g: (0, g)),
            pl.BlockSpec((seq_len, HEAD_WIDTH), lambda g: (0, key_at + g)),
            pl.BlockSpec((seq_len, HEAD_WIDTH), lambda g: (0, key_at + local_kv + g)),
            table,
            table,
        ],
        out_specs=pl.BlockSpec((seq_len, group * HEAD_WIDTH), lambda g: (0, g)),
        compiler_params=pltpu.CompilerParams(vmem_limit_bytes=24 << 20),
    )(product, product, product, cosine, sine)


def per_device(
    vis_rows,
    ln_gain,
    ln_bias,
    proj_weight,
    text_rows,
    attn_gain,
    w_query,
    key_value_weight,
    tile_counts,
    image_offsets,
):
    data_count = lax.axis_size("dp")
    data_index = lax.axis_index("dp")
    tensor_count = lax.axis_size("tensor")
    tensor_index = lax.axis_index("tensor")
    tile_rows, tile_tok, merge_count, part_width = vis_rows.shape
    feature = proj_weight.shape[0]
    part_model = proj_weight.shape[2]
    tokens = tile_rows * tile_tok
    mid = middle(data_count, tensor_count)
    far_count = data_count // NEAR
    far_here = far_count // tensor_count
    depth = w_query.shape[0]
    weights = (w_query, key_value_weight.reshape(depth, -1))
    tile = math.gcd(512, *(one.shape[1] for one in weights))
    chunks = sum(one.shape[1] for one in weights) // tile
    plan, have = gather_plan(far_count, chunks)

    tops = far_here // mid
    split = (tops, 2, mid, 2, feature)

    def arranged(rows):
        parts = rows.reshape(rows.shape[:-1] + split)
        lead = rows.ndim - 2
        order = (lead + 1, lead + 3) + tuple(range(lead)) + (lead + 2, lead + 4, lead, lead + 5)
        return parts.transpose(order).reshape((far_here,) + rows.shape[:lead] + (-1,))

    start = tensor_index * part_width
    gain = arranged(lax.dynamic_slice_in_dim(ln_gain, start, part_width, 1))
    bias = arranged(lax.dynamic_slice_in_dim(ln_bias, start, part_width, 1))
    rows_in = arranged(vis_rows.reshape(tokens, merge_count, part_width))
    proj = proj_weight.transpose(1, 0, 2).reshape(merge_count * feature, part_model)
    proj, normed, *gathered = front(
        rows_in, gain, bias, proj, *weights, tile, plan["front"], data_count, tensor_count, mid
    )
    image = project(normed, proj.reshape(-1, proj.shape[2]), mid)

    max_tiles = 2 * tile_rows
    tile_ends = jnp.cumsum(tile_counts)
    tile_firsts = tile_ends - tile_counts
    far_index = far_of(data_index, mid)
    sources = join(jnp.arange(NEAR, dtype=jnp.int32), far_index, mid)
    ranks = (sources[None, :] - tile_firsts[:, None]) % data_count
    taken = jnp.clip((tile_firsts[:, None] + ranks) // data_count, 0, tile_rows - 1)
    taken = taken + jnp.arange(NEAR, dtype=jnp.int32)[None, :] * tile_rows
    image = image.reshape(NEAR * tile_rows, tile_tok, image.shape[1])
    routed = image[taken].reshape(data_count, NEAR * tile_tok, image.shape[2])
    received = route(routed, mid).reshape(NEAR, data_count * tile_tok, image.shape[2])

    is_mine = jnp.arange(data_count, dtype=jnp.int32) == data_index
    my_first = jnp.sum(jnp.where(is_mine, tile_firsts, 0))
    my_count = jnp.sum(jnp.where(is_mine, tile_counts, 0))
    far_ids = jnp.arange(far_count, dtype=jnp.int32)[:, None]
    tile_ids = join(jnp.arange(NEAR, dtype=jnp.int32)[None, :], far_ids, mid).reshape(-1)
    order = (tile_ids - my_first) % data_count
    spots = image_offsets[0] + order * tile_tok
    spots = spots[:, None] + jnp.arange(tile_tok, dtype=jnp.int32)[None, :]
    spots = jnp.where((order < my_count)[:, None], spots, -1).reshape(1, -1)
    gain = lax.dynamic_slice_in_dim(attn_gain, tensor_index * part_model, part_model, 0)
    sequence, *gathered = sequences(
        spots, text_rows[0], received, gain[None, :], weights, gathered, tile,
        plan["sequence"], tensor_count, mid,
    )
    product = product_blocks(sequence, weights, gathered, tile, plan["product"], have, mid)
    context = attend(product, w_query.shape[1])
    return context[None]


def solution(mesh):
    in_specs = (
        P(None, "dp", None, "tensor"),
        P(),
        P(),
        P("dp", None, "tensor"),
        P("dp", None, "tensor"),
        P(),
        P("dp", "tensor"),
        P("dp", None, "tensor"),
        P(),
        P("dp"),
    )
    out_specs = P("dp", None, "tensor")
    return jax.shard_map(
        per_device, mesh=mesh, in_specs=in_specs, out_specs=out_specs, check_vma=False
    )
```

```python
import functools
import math

import jax
import jax.numpy as jnp
from jax import lax
from jax.experimental import pallas as pl
from jax.experimental.pallas import tpu as pltpu
from jax.sharding import PartitionSpec as P

QUERY_HEADS = 32
KEY_VALUE_HEADS = 8
HEAD_WIDTH = 128


vision_epsilon = 1e-06
decoder_epsilon = 1e-05
rope_base = 500000.0

MESH = pl.DeviceIdType.MESH
NEAR = 4


def near_of(index, mid):
    return index // (2 * mid) % 2 * 2 + index % 2


def far_of(index, mid):
    return index // (4 * mid) * mid + index // 2 % mid


def join(near, far, mid):
    return (far // mid * 2 + near // 2) * (2 * mid) + far % mid * 2 + near % 2


def middle_size(data_count, tensor_count):
    spare = int(math.log2(data_count)) - int(math.log2(tensor_count)) - 1
    return 1 << (min(2, spare) - 1)


def here(mid):
    data_index = lax.axis_index("dp")
    return near_of(data_index, mid), far_of(data_index, mid), lax.axis_index("tensor")


def meet(mid, near=True, far=True, twin=True):
    me, my_far, tensor_index = here(mid)
    far_count = lax.axis_size("dp") // NEAR
    tensor_count = lax.axis_size("tensor")
    targets = []
    if near:
        targets += [{"dp": join((me + s) % NEAR, my_far, mid)} for s in range(1, NEAR)]
    if far:
        targets += [{"dp": join(me, (my_far + s) % far_count, mid)} for s in range(1, far_count)]
    if twin:
        targets += [{"tensor": (tensor_index + s) % tensor_count} for s in range(1, tensor_count)]
    barrier = pltpu.get_barrier_semaphore()
    for target in targets:
        pl.semaphore_signal(barrier, inc=1, device_id=target, device_id_type=MESH)
    pl.semaphore_wait(barrier, len(targets))


def meet_all():
    data_index, data_count = lax.axis_index("dp"), lax.axis_size("dp")
    tensor_index, tensor_count = lax.axis_index("tensor"), lax.axis_size("tensor")
    targets = [{"dp": (data_index + s) % data_count} for s in range(1, data_count)]
    targets += [{"tensor": (tensor_index + s) % tensor_count} for s in range(1, tensor_count)]
    barrier = pltpu.get_barrier_semaphore()
    for target in targets:
        pl.semaphore_signal(barrier, inc=1, device_id=target, device_id_type=MESH)
    pl.semaphore_wait(barrier, len(targets))


def remote(src_ref, dst_ref, send_sem, recv_sem, device):
    return pltpu.make_async_remote_copy(
        src_ref=src_ref,
        dst_ref=dst_ref,
        send_sem=send_sem,
        recv_sem=recv_sem,
        device_id=device,
        device_id_type=MESH,
    )


def flip(index, bits):
    bit = 1
    while bit <= bits:
        if bits & bit:
            index = index + bit - 2 * bit * (index // bit % 2)
        bit *= 2
    return index


def gather_items(far_count):
    items, masks, bit = [], [0], far_count // 2
    while bit:
        items += [(bit, mask) for mask in masks]
        masks = masks + [mask | bit for mask in masks]
        bit //= 2
    return items


def gather_plan(far_count, chunks):
    third = chunks // 3
    high = far_count // 2
    items = gather_items(far_count)
    plan = {"front": [], "sequence": [], "product": []}
    have = {chunk: {0} for chunk in range(chunks)}
    for name, first, others in (
        ("front", range(third), range(2 * third)),
        ("sequence", range(third, 2 * third), range(2 * third, chunks)),
    ):
        held = {chunk: set(masks) for chunk, masks in have.items()}
        done = [job for jobs in plan.values() for job in jobs]
        for chunk in range(chunks):
            for bit, mask in items:
                wanted = (chunk in first) if bit == high else (chunk in others)
                if mask:
                    wanted = name == "sequence" and chunk < third and mask in held[chunk]
                if wanted and (bit, mask, chunk) not in done:
                    plan[name].append((bit, mask, chunk))
                    have[chunk].add(bit | mask)
    done = plan["front"] + plan["sequence"]
    for chunk in range(chunks):
        plan["product"] += [
            (bit, mask, chunk) for bit, mask in items if (bit, mask, chunk) not in done
        ]
    return plan, have


def chunk_at(chunk, tile, refs, lead):
    start = chunk * tile
    for ref in refs:
        width = ref.shape[-1]
        if start < width:
            part = pl.ds(start, tile)
            return ref.at[:, part] if lead is None else ref.at[lead, :, part]
        start -= width


def weight_copies(mid, tile, jobs, own_refs, got_refs, send, recv):
    me, my_far, _ = here(mid)
    copies = []
    for at, (bit, mask, chunk) in enumerate(jobs):
        block = flip(my_far, mask)
        source = chunk_at(chunk, tile, got_refs, block) if mask else chunk_at(
            chunk, tile, own_refs, None
        )
        copies.append(
            remote(
                source,
                chunk_at(chunk, tile, got_refs, block),
                send.at[at],
                recv.at[at],
                {"dp": join(me, flip(my_far, bit), mid)},
            )
        )
    return copies


class Halving:
    def __init__(self, bits, index, device, rows, out_ref, in_ref, acc_ref, own_ref, send, recv):
        self.bits, self.index, self.device, self.rows = bits, index, device, rows
        self.out_ref, self.in_ref, self.acc_ref, self.own_ref = out_ref, in_ref, acc_ref, own_ref
        self.send, self.recv = send, recv
        size = 1 << len(bits)
        self.stage_of = {
            mask: min(at for at, bit in enumerate(bits) if mask & bit) for mask in range(1, size)
        }
        later = [mask for mask in range(1, size) if self.stage_of[mask]]
        self.slot = {mask: at for at, mask in enumerate(later)}
        self.copies = []

    def masks(self, stage):
        return [mask for mask, at in self.stage_of.items() if at == stage]

    def start(self, stage):
        bit = self.bits[stage]
        for mask in self.masks(stage):
            copy = remote(
                self.out_ref.at[mask - 1],
                self.in_ref.at[mask - 1],
                self.send.at[mask - 1],
                self.recv.at[mask - 1],
                self.device(flip(self.index, bit)),
            )
            copy.start()
            self.copies.append((stage, copy))

    def receive(self, stage):
        for at, copy in self.copies:
            if at == stage:
                copy.wait_recv()
        rows, bit = self.rows, self.bits[stage]
        last = stage + 1 == len(self.bits)

        def add(at, carry):
            window = pl.ds(pl.multiple_of(at * rows, rows), rows)
            for mask in self.masks(stage):
                value = self.in_ref[mask - 1, window, :].astype(jnp.float32)
                rest = mask - bit
                if not rest:
                    self.own_ref[window, :] = self.own_ref[window, :] + value
                else:
                    value = self.acc_ref[self.slot[rest], window, :] + value
                    if self.stage_of[rest] == stage + 1:
                        self.out_ref[rest - 1, window, :] = value.astype(self.out_ref.dtype)
                    else:
                        self.acc_ref[self.slot[rest], window, :] = value
            return carry

        lax.fori_loop(0, self.own_ref.shape[0] // rows, add, 0)
        if not last:
            self.start(stage + 1)

    def finish(self):
        for _, copy in self.copies:
            copy.wait_send()


def front_kernel(mid, tile, jobs, x_ref, gain_ref, bias_ref, pw_ref, wq_ref, wkv_ref, pwg_ref,
                 vg_ref, gq_ref, gkv_ref, normed, stat_out, stat_in, pw_send, pw_recv, st_send,
                 st_recv, far_send, far_recv, near_send, near_recv, twin_send, twin_recv, w_send,
                 w_recv):
    merge_count, tokens, part_width = x_ref.shape
    blocks, _, width = normed.shape
    far_count = vg_ref.shape[1]
    rows, wide = pwg_ref.shape[1:]
    feature = rows // merge_count
    tensor_count = lax.axis_size("tensor")
    me, my_far, tensor_index = here(mid)
    meet(mid)
    pw_copies = []
    for step in range(1, NEAR):
        target = (me + step) % NEAR
        copy = remote(
            pw_ref.at[:, pl.ds(pl.multiple_of(target * wide, wide), wide)],
            pwg_ref.at[me],
            pw_send.at[step - 1],
            pw_recv.at[step - 1],
            {"dp": join(target, my_far, mid)},
        )
        copy.start()
        pw_copies.append(copy)
    w_copies = weight_copies(
        mid, tile, jobs, (wq_ref, wkv_ref), (gq_ref, gkv_ref), w_send, w_recv
    )
    early = len(w_copies) // 3
    for copy in w_copies[:early]:
        copy.start()

    count = merge_count * part_width
    total = jnp.zeros((tokens, 1), jnp.float32)
    for at in range(merge_count):
        total = total + jnp.sum(x_ref[at].astype(jnp.float32), axis=-1, keepdims=True)
    mean = total / count
    spread = jnp.zeros((tokens, 1), jnp.float32)
    for at in range(merge_count):
        centered = x_ref[at].astype(jnp.float32) - mean
        spread = spread + jnp.sum(centered * centered, axis=-1, keepdims=True)
    stat_out[0] = jnp.broadcast_to(mean, stat_out.shape[1:])
    stat_out[1] = jnp.broadcast_to(spread, stat_out.shape[1:])
    stat_copies = []
    for step in range(1, tensor_count):
        copy = remote(
            stat_out,
            stat_in.at[step - 1],
            st_send.at[step - 1],
            st_recv.at[step - 1],
            {"tensor": (tensor_index + step) % tensor_count},
        )
        copy.start()
        stat_copies.append(copy)
    for copy in stat_copies:
        copy.wait_recv()
    means, spreads = [mean], [spread]
    for step in range(1, tensor_count):
        means.append(stat_in[step - 1, 0][:, :1])
        spreads.append(stat_in[step - 1, 1][:, :1])
    average = sum(means) / tensor_count
    variance = sum(s + count * (one - average) * (one - average) for s, one in zip(spreads, means))
    scale = lax.rsqrt(variance / (count * tensor_count) + vision_epsilon)
    merged = [
        (x_ref[at].astype(jnp.float32) - average) * scale * gain_ref[pl.ds(at, 1)]
        + bias_ref[pl.ds(at, 1)]
        for at in range(merge_count)
    ]
    far_copies = []
    for at in range(blocks):
        pieces = []
        for block in range(NEAR):
            start = join(block, at, mid) * feature
            pieces += [one[:, start : start + feature] for one in merged]
        normed[at] = jnp.concatenate(pieces, axis=1).astype(normed.dtype)
        goal = tensor_index * blocks + at
        mine = goal == my_far
        copy = remote(
            normed.at[at],
            vg_ref.at[me, my_far],
            far_send.at[at],
            far_recv.at[my_far],
            {"dp": join(me, goal, mid)},
        )
        pl.when(jnp.logical_not(mine))(copy.start)
        far_copies.append((mine, copy))

        @pl.when(mine)
        def _():
            vg_ref[me, my_far] = normed[at]

    for copy in w_copies[early:]:
        copy.start()
    holder = my_far // blocks == tensor_index

    def twin_copy(ahead, mask):
        block = flip(me, mask)
        return remote(
            vg_ref.at[block],
            vg_ref.at[block],
            twin_send.at[ahead - 1, mask],
            twin_recv.at[mask],
            {"tensor": (tensor_index + ahead) % tensor_count},
        )

    def near_copy(bit, mask):
        block = flip(me, mask)
        return remote(
            vg_ref.at[block],
            vg_ref.at[block],
            near_send.at[(bit | mask) - 1],
            near_recv.at[(bit | mask) - 1],
            {"dp": join(flip(me, bit), my_far, mid)},
        )

    @pl.when(holder)
    def _():
        for step in range(1, far_count):
            source = (my_far + step) % far_count
            remote(
                normed.at[0],
                vg_ref.at[me, source],
                far_send.at[0],
                far_recv.at[source],
                {"dp": join(me, source, mid)},
            ).wait_recv()
        near_copies = {mask | bit: near_copy(bit, mask) for bit, mask in ((2, 0), (1, 0), (1, 2))}
        twin_copies = []
        near_copies[2].start()
        near_copies[1].start()
        for mask in (0, 2, 1, 3):
            if mask:
                near_copies[mask].wait_recv()
            if mask == 2:
                near_copies[3].start()
            for ahead in range(1, tensor_count):
                copy = twin_copy(ahead, mask)
                copy.start()
                twin_copies.append(copy)
        for copy in list(near_copies.values()) + twin_copies:
            copy.wait_send()

    def keep(at, carry):
        window = pl.ds(pl.multiple_of(at * 16, 16), 16)
        pwg_ref[me, window] = pw_ref[window, pl.ds(pl.multiple_of(me * wide, wide), wide)]
        return carry

    lax.fori_loop(0, rows // 16, keep, 0)

    @pl.when(jnp.logical_not(holder))
    def _():
        for step in range(NEAR):
            twin_copy(1, step).wait_recv()

    for mine, copy in far_copies:
        pl.when(jnp.logical_not(mine))(copy.wait_send)
    for copy in stat_copies:
        copy.wait_send()
    for copy in pw_copies + w_copies:
        copy.wait()


def front(x, gain, bias, proj, w_query, w_kv, tile, jobs, data_count, tensor_count, mid):
    merge_count, tokens, part_width = x.shape
    far_count = data_count // NEAR
    blocks = far_count // tensor_count
    width = merge_count * part_width // blocks
    rows, columns = proj.shape
    vmem = pl.BlockSpec(memory_space=pltpu.VMEM)
    anywhere = pl.BlockSpec(memory_space=pltpu.HBM)
    dma = pltpu.SemaphoreType.DMA
    return pl.pallas_call(
        functools.partial(front_kernel, mid, tile, jobs),
        out_shape=(
            jax.ShapeDtypeStruct((NEAR, rows, columns // NEAR), proj.dtype),
            jax.ShapeDtypeStruct((NEAR, far_count, tokens, width), x.dtype),
            jax.ShapeDtypeStruct((far_count,) + w_query.shape, w_query.dtype),
            jax.ShapeDtypeStruct((far_count,) + w_kv.shape, w_kv.dtype),
        ),
        in_specs=[vmem] * 4 + [anywhere] * 2,
        out_specs=(vmem, vmem, anywhere, anywhere),
        scratch_shapes=[
            pltpu.VMEM((blocks, tokens, width), x.dtype),
            pltpu.VMEM((2, tokens, 128), jnp.float32),
            pltpu.VMEM((tensor_count - 1, 2, tokens, 128), jnp.float32),
            dma((NEAR - 1,)),
            dma((NEAR - 1,)),
            dma((tensor_count - 1,)),
            dma((tensor_count - 1,)),
            dma((blocks,)),
            dma((far_count,)),
            dma((NEAR - 1,)),
            dma((NEAR - 1,)),
            dma((tensor_count - 1, NEAR)),
            dma((NEAR,)),
            dma((len(jobs),)),
            dma((len(jobs),)),
        ],
        compiler_params=pltpu.CompilerParams(
            collective_id=0, has_side_effects=True, vmem_limit_bytes=40 << 20
        ),
        cost_estimate=pl.CostEstimate(flops=0, bytes_accessed=80 << 20, transcendentals=0),
    )(x, gain, bias, proj, w_query, w_kv)


def middle_kernel(mid, tile, span, w_tile, jobs, vg_ref, pw_ref, pick_ref, rows_ref, spot_ref, text_ref,
                  gain_ref, wq_ref, wkv_ref, gq_in, gkv_in, a_ref, gq_ref, gkv_ref, own, acc, out,
                  held_ref, t_send, t_recv, tiles, got, r_send, r_recv, seq, sums, sums_in,
                  leaving, st_send, st_recv, near_send, near_recv, twin_send, twin_recv, w_send,
                  w_recv):
    near, far_count, tokens, width = vg_ref.shape
    _, seq_len, depth = a_ref.shape
    chunks = own.shape[0]
    data_index, data_count = lax.axis_index("dp"), lax.axis_size("dp")
    tensor_count = lax.axis_size("tensor")
    held = depth // tensor_count
    model_width = text_ref.shape[1] * tensor_count
    wide = got.shape[3]
    spots = spot_ref.shape[1]
    early = seq_len - span
    me, my_far, tensor_index = here(mid)
    shift = held // (far_count // tensor_count)
    bits = []
    while 1 << len(bits) < far_count:
        bits.append(1 << len(bits))
    meet_all()
    w_copies = weight_copies(
        mid, w_tile, jobs, (wq_ref, wkv_ref), (gq_ref, gkv_ref), w_send, w_recv
    )
    half = [copy for copy, job in zip(w_copies, jobs) if job[0] == far_count // 2]
    rest = [copy for copy, job in zip(w_copies, jobs) if job[0] != far_count // 2]
    for copy in half[:1]:
        copy.start()

    def compute(mask, chunk, dst_ref):
        term = jnp.dot(
            vg_ref[:, flip(my_far, mask)].reshape(near * tokens, width),
            pw_ref[:, pl.ds(chunk * tile, tile)],
            preferred_element_type=jnp.float32,
        )
        dst_ref[...] = term.astype(dst_ref.dtype)

    parts = []
    for chunk in range(chunks):
        one = Halving(
            bits, my_far, lambda far: {"dp": join(me, far, mid)}, 32, out.at[chunk],
            held_ref.at[chunk], acc.at[chunk], own.at[chunk], t_send.at[chunk], t_recv.at[chunk],
        )
        for mask in one.masks(0):
            compute(mask, chunk, out.at[chunk, mask - 1])
        one.start(0)
        parts.append(one)
    for copy in rest:
        copy.start()
    for chunk, one in enumerate(parts):
        for mask, slot in one.slot.items():
            compute(mask, chunk, acc.at[chunk, slot])
        compute(0, chunk, own.at[chunk])

    rows = math.gcd(early, span)

    def fill(start, image):
        window = pl.ds(pl.multiple_of(start, rows), rows)
        place = lax.broadcasted_iota(jnp.int32, (rows, seq_len), 1)
        chosen = jnp.where(place == rows_ref[window, :], 1.0, 0.0).astype(jnp.bfloat16)
        if image:
            slots = lax.broadcasted_iota(jnp.int32, (rows, spots), 0) + (start - early)
            drawn = jnp.where(slots == spot_ref[...], 1.0, 0.0)
            is_image = jnp.max(drawn, axis=-1, keepdims=True) > 0.5
            drawn = drawn.astype(jnp.bfloat16)
        squares = jnp.zeros((rows, 1), jnp.float32)
        for part in range(near):
            lanes = pl.ds(part * wide, wide)
            value = jnp.dot(chosen, text_ref[:, lanes], preferred_element_type=jnp.float32)
            if image:
                tokens_here = got[part].reshape(spots, wide)
                tile_rows = jnp.dot(drawn, tokens_here, preferred_element_type=jnp.float32)
                value = jnp.where(is_image, tile_rows, value)
            seq[window, lanes] = value.astype(seq.dtype)
            squares = squares + jnp.sum(value * value, axis=-1, keepdims=True)
        sums[window, :] = jnp.broadcast_to(squares, (rows, sums.shape[1]))

    def share(phase, low, count):
        window = pl.ds(low, count)
        copies = []
        for step in range(1, tensor_count):
            copy = remote(
                sums.at[window],
                sums_in.at[step - 1, window],
                st_send.at[phase, step - 1],
                st_recv.at[phase, step - 1],
                {"tensor": (tensor_index + step) % tensor_count},
            )
            copy.start()
            copies.append(copy)
        return copies

    def lanes_of(owner):
        return pl.ds(pl.multiple_of(owner * held, held), held)

    fine = math.gcd(rows, 32)

    def norm(target, low, count, store):
        def one(at, carry):
            window = pl.ds(pl.multiple_of(low + at * fine, fine), fine)
            squares = sums[window, :][:, :1]
            for step in range(1, tensor_count):
                squares = squares + sums_in[step - 1, window, :][:, :1]
            scale = lax.rsqrt(squares / model_width + decoder_epsilon)
            for part in range(held // shift):
                lanes = pl.ds(pl.multiple_of(join(target, part, mid) * shift, shift), shift)
                value = seq[window, lanes].astype(jnp.float32) * scale * gain_ref[:, lanes]
                store(window, part * shift, value.astype(jnp.bfloat16))
            return carry

        lax.fori_loop(0, count // fine, one, 0)

    def stay(window, start, value):
        lanes = pl.ds(pl.multiple_of(tensor_index * held + start, shift), shift)
        a_ref[me, window, lanes] = value

    def spread(phase, low, count):
        window = pl.ds(low, count)
        copies = []
        for step in range(1, NEAR):

            def leave(window, start, value):
                leaving[step - 1, window, pl.ds(start, shift)] = value

            norm(flip(me, step), low, count, leave)
            copy = remote(
                leaving.at[step - 1, window],
                a_ref.at[me, window, lanes_of(tensor_index)],
                near_send.at[phase, step - 1],
                near_recv.at[phase, step - 1],
                {"dp": join(flip(me, step), my_far, mid)},
            )
            copy.start()
            copies.append(copy)
        norm(me, low, count, stay)
        return copies

    def twin_copy(phase, low, count, ahead, step, owner):
        block, window = flip(me, step), pl.ds(low, count)
        return remote(
            a_ref.at[block, window, lanes_of(owner)],
            a_ref.at[block, window, lanes_of(owner)],
            twin_send.at[phase, ahead - 1, step],
            twin_recv.at[phase, ahead - 1, step],
            {"tensor": (tensor_index + ahead) % tensor_count},
        )

    def pass_on(phase, low, count, near_copies):
        copies = []
        for step in range(NEAR):
            if step:
                near_copies[step - 1].wait_recv()
            for ahead in range(1, tensor_count):
                copy = twin_copy(phase, low, count, ahead, step, tensor_index)
                copy.start()
                copies.append(copy)
        return copies

    def collect(phase, low, count):
        for ahead in range(1, tensor_count):
            for step in range(NEAR):
                owner = (tensor_index + tensor_count - ahead) % tensor_count
                twin_copy(phase, low, count, ahead, step, owner).wait_recv()

    for start in range(0, early, rows):
        fill(start, False)
    stat_copies = share(0, 0, early)
    for one in parts:
        one.receive(0)
    for copy in stat_copies:
        copy.wait_recv()
    near_early = spread(0, 0, early)
    for stage in range(1, len(bits)):
        for one in parts:
            one.receive(stage)

    place = lax.broadcasted_iota(jnp.int32, (pick_ref.shape[0], near * tokens), 1)
    chosen = jnp.where(place == pick_ref[...], 1.0, 0.0).astype(jnp.bfloat16)
    for chunk in range(chunks):
        image = own[chunk].astype(jnp.bfloat16)
        sorted_rows = jnp.dot(chosen, image, preferred_element_type=jnp.float32)
        tiles[:, :, pl.ds(chunk * tile, tile)] = sorted_rows.astype(tiles.dtype).reshape(
            tiles.shape[0], tiles.shape[1], tile
        )
    route_copies = []
    for step in range(1, data_count):
        target = (data_index + step) % data_count
        copy = remote(
            tiles.at[target],
            got.at[me, my_far],
            r_send.at[step - 1],
            r_recv.at[step - 1],
            {"dp": target},
        )
        copy.start()
        route_copies.append(copy)
    for copy in half[1:]:
        copy.start()
    got[me, my_far] = tiles[data_index]
    twin_early = pass_on(0, 0, early, near_early)
    for copy in route_copies:
        copy.wait_recv()
    for start in range(early, seq_len, rows):
        fill(start, True)
    late_copies = share(1, early, span)
    for copy in late_copies:
        copy.wait_recv()
    near_late = spread(1, early, span)
    twin_late = pass_on(1, early, span, near_late)
    collect(0, 0, early)
    collect(1, early, span)
    for copy in near_early + near_late + twin_early + twin_late + stat_copies + late_copies:
        copy.wait_send()
    for copy in route_copies:
        copy.wait_send()
    for one in parts:
        one.finish()
    for copy in w_copies:
        copy.wait()


def middle_part(vg, pw, pick, rows, spots, span, text, gain, weights, gathered, w_tile, jobs, mid):
    near, far_count, tokens, width = vg.shape
    columns = pw.shape[1]
    tensor_count = lax.axis_size("tensor")
    data_count = lax.axis_size("dp")
    tile = math.gcd(columns, 512)
    chunks = columns // tile
    seq_len, part_model = text.shape
    held = part_model // NEAR
    sent = pick.shape[0] // data_count
    vmem = pl.BlockSpec(memory_space=pltpu.VMEM)
    anywhere = pl.BlockSpec(memory_space=pltpu.HBM)
    dma = pltpu.SemaphoreType.DMA
    return pl.pallas_call(
        functools.partial(middle_kernel, mid, tile, span, w_tile, jobs),
        out_shape=(jax.ShapeDtypeStruct((NEAR, seq_len, held * tensor_count), text.dtype),)
        + tuple(jax.ShapeDtypeStruct(one.shape, one.dtype) for one in gathered),
        in_specs=[vmem] * 7 + [anywhere] * 4,
        out_specs=(vmem, anywhere, anywhere),
        input_output_aliases={9: 1, 10: 2},
        scratch_shapes=[
            pltpu.VMEM((chunks, near * tokens, tile), jnp.float32),
            pltpu.VMEM((chunks, far_count // 2 - 1, near * tokens, tile), jnp.float32),
            pltpu.VMEM((chunks, far_count - 1, near * tokens, tile), vg.dtype),
            pltpu.VMEM((chunks, far_count - 1, near * tokens, tile), vg.dtype),
            dma((chunks, far_count - 1)),
            dma((chunks, far_count - 1)),
            pltpu.VMEM((data_count, sent, columns), vg.dtype),
            pltpu.VMEM((NEAR, far_count, sent, columns), vg.dtype),
            dma((data_count - 1,)),
            dma((data_count - 1,)),
            pltpu.VMEM((seq_len, part_model), text.dtype),
            pltpu.VMEM((seq_len, 128), jnp.float32),
            pltpu.VMEM((tensor_count - 1, seq_len, 128), jnp.float32),
            pltpu.VMEM((NEAR - 1, seq_len, held), text.dtype),
            dma((2, tensor_count - 1)),
            dma((2, tensor_count - 1)),
            dma((2, NEAR - 1)),
            dma((2, NEAR - 1)),
            dma((2, tensor_count - 1, NEAR)),
            dma((2, tensor_count - 1, NEAR)),
            dma((len(jobs),)),
            dma((len(jobs),)),
        ],
        compiler_params=pltpu.CompilerParams(
            collective_id=1, has_side_effects=True, vmem_limit_bytes=48 << 20
        ),
        cost_estimate=pl.CostEstimate(
            flops=2 * far_count * near * tokens * width * columns,
            bytes_accessed=100 << 20,
            transcendentals=0,
        ),
    )(vg, pw, pick, rows, spots, text, gain, *weights, *gathered)


def product_kernel(mid, tile, jobs, have, a_ref, wq_ref, wkv_ref, gq_ref, gkv_ref, o_ref, w, acc,
                   out, held, send, recv, w_send, w_recv, load_sem):
    _, seq_len, _ = a_ref.shape
    depth = wq_ref.shape[0]
    far_count = gq_ref.shape[0]
    me, my_far, _ = here(mid)
    chunks = len(have)
    own_refs, got_refs = (wq_ref, wkv_ref), (gq_ref, gkv_ref)

    def place(mask, chunk):
        rows = pl.ds(pl.multiple_of(flip(my_far, mask) * depth, depth), depth)
        return w.at[rows, pl.ds(chunk * tile, tile)]

    def local(mask, chunk):
        if mask:
            return chunk_at(chunk, tile, got_refs, flip(my_far, mask))
        return chunk_at(chunk, tile, own_refs, None)

    loads = {}
    for chunk in range(chunks):
        for mask in sorted(have[chunk]):
            loads[mask, chunk] = pltpu.make_async_copy(
                local(mask, chunk), place(mask, chunk), load_sem.at[chunk, mask]
            )
            loads[mask, chunk].start()

    meet(mid, twin=False)
    arriving, waiting = {}, {chunk: [] for chunk in range(chunks)}
    for at, (bit, mask, chunk) in enumerate(jobs):
        kept = mask in have[chunk]
        copy = remote(
            local(mask, chunk) if kept else place(mask, chunk),
            place(mask, chunk),
            w_send.at[at],
            w_recv.at[at],
            {"dp": join(me, flip(my_far, bit), mid)},
        )
        arriving[bit | mask, chunk] = copy
        if kept:
            copy.start()
        else:
            waiting[chunk].append((mask, copy))
    seen = set()

    def ensure(mask, chunk):
        if (mask, chunk) not in seen:
            seen.add((mask, chunk))
            if (mask, chunk) in loads:
                loads[mask, chunk].wait()
            else:
                arriving[mask, chunk].wait_recv()

    def forward(chunk):
        for mask, copy in waiting.pop(chunk, ()):
            ensure(mask, chunk)
            copy.start()

    sums = []
    third = chunks // 3

    def compute(chunk):
        forward(chunk)
        for mask in range(far_count):
            ensure(mask, chunk)
        part = pl.ds(chunk * tile, tile)
        bits = (2, 1) if chunk % 2 and chunk < 2 * third else (1, 2)
        one = Halving(
            bits, me, lambda near: {"dp": join(near, my_far, mid)}, math.gcd(seq_len, 32),
            out.at[chunk], held.at[chunk], acc.at[chunk], o_ref.at[:, part], send.at[chunk],
            recv.at[chunk],
        )

        def fill(mask, dst_ref):
            term = jnp.dot(
                a_ref[flip(me, mask)], w[:, part], preferred_element_type=jnp.float32
            )
            dst_ref[...] = term.astype(dst_ref.dtype)

        for mask in one.masks(0):
            fill(mask, out.at[chunk, mask - 1])
        one.start(0)
        for mask, slot in one.slot.items():
            fill(mask, acc.at[chunk, slot])
        fill(0, o_ref.at[:, part])
        sums.append(one)

    done = {0: 0, 1: 0}

    def reduce(stage, upto):
        for one in sums[done[stage] : upto]:
            one.receive(stage)
        done[stage] = max(done[stage], upto)

    for chunk in range(2 * third):
        compute(chunk)
    reduce(0, third)
    for chunk in range(2 * third, chunks):
        forward(chunk)
        reduce(0, 2 * third)
        if chunk > 2 * third:
            reduce(1, 2 * third)
        compute(chunk)
    reduce(0, chunks)
    reduce(1, chunks)
    for one in sums:
        one.finish()
    for copy in arriving.values():
        copy.wait_send()


def product_blocks(a, weights, gathered, tile, jobs, have, mid):
    _, seq_len, depth = a.shape
    columns = sum(one.shape[1] for one in weights)
    chunks = columns // tile
    vmem = pl.BlockSpec(memory_space=pltpu.VMEM)
    anywhere = pl.BlockSpec(memory_space=pltpu.HBM)
    far_count = gathered[0].shape[0]
    dma = pltpu.SemaphoreType.DMA
    return pl.pallas_call(
        functools.partial(product_kernel, mid, tile, jobs, have),
        out_shape=jax.ShapeDtypeStruct((seq_len, columns), jnp.float32),
        in_specs=[vmem] + [anywhere] * 4,
        out_specs=vmem,
        scratch_shapes=[
            pltpu.VMEM((depth, columns), jnp.bfloat16),
            pltpu.VMEM((chunks, NEAR // 2 - 1, seq_len, tile), jnp.float32),
            pltpu.VMEM((chunks, NEAR - 1, seq_len, tile), jnp.bfloat16),
            pltpu.VMEM((chunks, NEAR - 1, seq_len, tile), jnp.bfloat16),
            dma((chunks, NEAR - 1)),
            dma((chunks, NEAR - 1)),
            dma((len(jobs),)),
            dma((len(jobs),)),
            dma((chunks, far_count)),
        ],
        compiler_params=pltpu.CompilerParams(
            collective_id=2, has_side_effects=True, vmem_limit_bytes=56 << 20
        ),
        cost_estimate=pl.CostEstimate(
            flops=2 * NEAR * seq_len * depth * columns,
            bytes_accessed=200 << 20,
            transcendentals=0,
        ),
    )(a, *weights, *gathered)


def attend_kernel(group, q_ref, k_ref, v_ref, cos_ref, sin_ref, down_ref, across_ref, o_ref):
    cosine, sine = cos_ref[...], sin_ref[...]

    def turn(rows):
        return (rows * cosine + pltpu.roll(rows, HEAD_WIDTH // 2, 1) * sine).astype(jnp.bfloat16)

    key_rows = turn(k_ref[...])
    value_rows = v_ref[...].astype(jnp.bfloat16)
    seq_len = key_rows.shape[0]
    allowed = down_ref[...] >= across_ref[...]
    row_at = lax.broadcasted_iota(jnp.int32, (seq_len, seq_len), 0)
    home = jnp.where(row_at == across_ref[...], 1.0, 0.0).astype(jnp.bfloat16)
    for head in range(group):
        part = pl.ds(head * HEAD_WIDTH, HEAD_WIDTH)
        query_rows = turn(q_ref[:, part])
        scores = lax.dot_general(
            query_rows, key_rows, (((1,), (1,)), ((), ())), preferred_element_type=jnp.float32
        ) * HEAD_WIDTH ** (-0.5)
        scores = jnp.where(allowed, scores, -1e30)
        exponentials = jnp.exp(scores - jnp.max(scores, axis=-1, keepdims=True))
        weights = exponentials / jnp.sum(exponentials, axis=-1, keepdims=True)
        context = jnp.dot(
            weights.astype(jnp.bfloat16), value_rows, preferred_element_type=jnp.float32
        )
        ordered = jnp.dot(
            home, context.astype(jnp.bfloat16), preferred_element_type=jnp.float32
        )
        o_ref[:, part] = ordered.astype(o_ref.dtype)


def attend(product, positions, part_query):
    seq_len, columns = product.shape
    group = QUERY_HEADS // KEY_VALUE_HEADS
    local_kv = part_query // HEAD_WIDTH // group
    key_at = part_query // HEAD_WIDTH
    half_width = HEAD_WIDTH // 2
    exponents = jnp.arange(half_width, dtype=jnp.float32) * (2.0 / HEAD_WIDTH)
    frequency = rope_base ** (-exponents)
    angles = positions.astype(jnp.float32)[:, None] * frequency[None, :]
    cosine, sine = jnp.cos(angles), jnp.sin(angles)
    cosine = jnp.concatenate([cosine, cosine], axis=1)
    sine = jnp.concatenate([-sine, sine], axis=1)
    table = pl.BlockSpec((seq_len, HEAD_WIDTH), lambda g: (0, 0))
    return pl.pallas_call(
        functools.partial(attend_kernel, group),
        grid=(local_kv,),
        out_shape=jax.ShapeDtypeStruct((seq_len, part_query), jnp.bfloat16),
        in_specs=[
            pl.BlockSpec((seq_len, group * HEAD_WIDTH), lambda g: (0, g)),
            pl.BlockSpec((seq_len, HEAD_WIDTH), lambda g: (0, key_at + g)),
            pl.BlockSpec((seq_len, HEAD_WIDTH), lambda g: (0, key_at + local_kv + g)),
            table,
            table,
            pl.BlockSpec((seq_len, 1), lambda g: (0, 0)),
            pl.BlockSpec((1, seq_len), lambda g: (0, 0)),
        ],
        out_specs=pl.BlockSpec((seq_len, group * HEAD_WIDTH), lambda g: (0, g)),
        compiler_params=pltpu.CompilerParams(vmem_limit_bytes=24 << 20),
    )(product, product, product, cosine, sine, positions[:, None], positions[None, :])


def per_device(
    vis_rows,
    ln_gain,
    ln_bias,
    proj_weight,
    text_rows,
    attn_gain,
    w_query,
    key_value_weight,
    tile_counts,
    image_offsets,
):
    data_count = lax.axis_size("dp")
    data_index = lax.axis_index("dp")
    tensor_count = lax.axis_size("tensor")
    tensor_index = lax.axis_index("tensor")
    tile_rows, tile_tok, merge_count, part_width = vis_rows.shape
    feature = proj_weight.shape[0]
    part_model = proj_weight.shape[2]
    tokens = tile_rows * tile_tok
    mid = middle_size(data_count, tensor_count)
    far_count = data_count // NEAR
    far_here = far_count // tensor_count
    depth = w_query.shape[0]
    weights = (w_query, key_value_weight.reshape(depth, -1))
    tile = math.gcd(512, *(one.shape[1] for one in weights))
    chunks = sum(one.shape[1] for one in weights) // tile
    plan, have = gather_plan(far_count, chunks)

    start = tensor_index * part_width
    gain = lax.dynamic_slice_in_dim(ln_gain, start, part_width, 1)
    bias = lax.dynamic_slice_in_dim(ln_bias, start, part_width, 1)
    rows_in = vis_rows.reshape(tokens, merge_count, part_width).transpose(1, 0, 2)
    proj = proj_weight.transpose(1, 0, 2).reshape(merge_count * feature, part_model)
    proj, normed, *gathered = front(
        rows_in, gain, bias, proj, *weights, tile, plan["front"], data_count, tensor_count, mid
    )

    max_tiles = 2 * tile_rows
    tile_ends = jnp.cumsum(tile_counts)
    tile_firsts = tile_ends - tile_counts
    far_index = far_of(data_index, mid)
    sources = join(jnp.arange(NEAR, dtype=jnp.int32), far_index, mid)
    ranks = (sources[None, :] - tile_firsts[:, None]) % data_count
    taken = jnp.clip((tile_firsts[:, None] + ranks) // data_count, 0, tile_rows - 1)
    taken = taken + jnp.arange(NEAR, dtype=jnp.int32)[None, :] * tile_rows
    token_at = jnp.arange(tile_tok, dtype=jnp.int32)
    pick = (taken.reshape(-1, 1) * tile_tok + token_at[None, :]).reshape(-1, 1)

    is_mine = jnp.arange(data_count, dtype=jnp.int32) == data_index
    my_first = jnp.sum(jnp.where(is_mine, tile_firsts, 0))
    my_count = jnp.sum(jnp.where(is_mine, tile_counts, 0))
    far_ids = jnp.arange(far_count, dtype=jnp.int32)[:, None]
    tile_ids = join(jnp.arange(NEAR, dtype=jnp.int32)[None, :], far_ids, mid).reshape(-1)
    order = (tile_ids - my_first) % data_count
    spots = order[:, None] * tile_tok + token_at[None, :]
    spots = jnp.where((order < my_count)[:, None], spots, -1).reshape(1, -1)

    seq_len = text_rows.shape[1]
    image_span = max_tiles * tile_tok
    offset = image_offsets[0]
    outside = jnp.arange(seq_len - image_span, dtype=jnp.int32)
    outside = jnp.where(outside < offset, outside, outside + image_span)
    positions = jnp.concatenate([outside, offset + jnp.arange(image_span, dtype=jnp.int32)])
    gain = lax.dynamic_slice_in_dim(attn_gain, tensor_index * part_model, part_model, 0)
    sequence, *gathered = middle_part(
        normed, proj.reshape(-1, proj.shape[2]), pick, positions[:, None], spots, image_span,
        text_rows[0], gain[None, :], weights, gathered, tile, plan["sequence"], mid,
    )
    product = product_blocks(sequence, weights, gathered, tile, plan["product"], have, mid)
    context = attend(product, positions, w_query.shape[1])
    return context[None]


def solution(mesh):
    in_specs = (
        P(None, "dp", None, "tensor"),
        P(),
        P(),
        P("dp", None, "tensor"),
        P("dp", None, "tensor"),
        P(),
        P("dp", "tensor"),
        P("dp", None, "tensor"),
        P(),
        P("dp"),
    )
    out_specs = P("dp", None, "tensor")
    return jax.shard_map(
        per_device, mesh=mesh, in_specs=in_specs, out_specs=out_specs, check_vma=False
    )
```

```python
import functools
import math

import jax
import jax.numpy as jnp
from jax import lax
from jax.experimental import pallas as pl
from jax.experimental.pallas import tpu as pltpu
from jax.sharding import PartitionSpec as P

QUERY_HEADS = 32
KEY_VALUE_HEADS = 8
HEAD_WIDTH = 128


vision_epsilon = 1e-06
decoder_epsilon = 1e-05
rope_base = 500000.0

MESH = pl.DeviceIdType.MESH
NEAR = 4


def near_of(index, mid):
    return index // (2 * mid) % 2 * 2 + index % 2


def far_of(index, mid):
    return index // (4 * mid) * mid + index // 2 % mid


def join(near, far, mid):
    return (far // mid * 2 + near // 2) * (2 * mid) + far % mid * 2 + near % 2


def middle_size(data_count, tensor_count):
    spare = int(math.log2(data_count)) - int(math.log2(tensor_count)) - 1
    return 1 << (min(2, spare) - 1)


def here(mid):
    data_index = lax.axis_index("dp")
    return near_of(data_index, mid), far_of(data_index, mid), lax.axis_index("tensor")


def meet(mid, near=True, far=True, twin=True):
    me, my_far, tensor_index = here(mid)
    far_count = lax.axis_size("dp") // NEAR
    tensor_count = lax.axis_size("tensor")
    targets = []
    if near:
        targets += [{"dp": join((me + s) % NEAR, my_far, mid)} for s in range(1, NEAR)]
    if far:
        targets += [{"dp": join(me, (my_far + s) % far_count, mid)} for s in range(1, far_count)]
    if twin:
        targets += [{"tensor": (tensor_index + s) % tensor_count} for s in range(1, tensor_count)]
    barrier = pltpu.get_barrier_semaphore()
    for target in targets:
        pl.semaphore_signal(barrier, inc=1, device_id=target, device_id_type=MESH)
    pl.semaphore_wait(barrier, len(targets))


def meet_all():
    data_index, data_count = lax.axis_index("dp"), lax.axis_size("dp")
    tensor_index, tensor_count = lax.axis_index("tensor"), lax.axis_size("tensor")
    targets = [{"dp": (data_index + s) % data_count} for s in range(1, data_count)]
    targets += [{"tensor": (tensor_index + s) % tensor_count} for s in range(1, tensor_count)]
    barrier = pltpu.get_barrier_semaphore()
    for target in targets:
        pl.semaphore_signal(barrier, inc=1, device_id=target, device_id_type=MESH)
    pl.semaphore_wait(barrier, len(targets))


def remote(src_ref, dst_ref, send_sem, recv_sem, device):
    return pltpu.make_async_remote_copy(
        src_ref=src_ref,
        dst_ref=dst_ref,
        send_sem=send_sem,
        recv_sem=recv_sem,
        device_id=device,
        device_id_type=MESH,
    )


def flip(index, bits):
    bit = 1
    while bit <= bits:
        if bits & bit:
            index = index + bit - 2 * bit * (index // bit % 2)
        bit *= 2
    return index


def gather_items(far_count):
    items, masks, bit = [], [0], far_count // 2
    while bit:
        items += [(bit, mask) for mask in masks]
        masks = masks + [mask | bit for mask in masks]
        bit //= 2
    return items


def gather_plan(far_count, chunks):
    third = chunks // 3
    high = far_count // 2
    items = gather_items(far_count)
    plan = {"front": [], "sequence": [], "product": []}
    have = {chunk: {0} for chunk in range(chunks)}
    plan["front"] = [(high, 0, chunk) for chunk in range(third)]
    plan["sequence"] = [(high, 0, chunk) for chunk in range(third, 2 * third)]
    plan["sequence"] += [
        (bit, 0, chunk) for bit, mask in items if not mask and bit != high
        for chunk in range(chunks)
    ]
    plan["sequence"] += [
        (bit, mask, chunk) for bit, mask in items if mask == high for chunk in range(third)
    ]
    for bit, mask, chunk in plan["front"] + plan["sequence"]:
        have[chunk].add(bit | mask)
    done = plan["front"] + plan["sequence"]
    for chunk in range(chunks):
        plan["product"] += [
            (bit, mask, chunk) for bit, mask in items if (bit, mask, chunk) not in done
        ]
    return plan, have


def chunk_at(chunk, tile, refs, lead):
    start = chunk * tile
    for ref in refs:
        width = ref.shape[-1]
        if start < width:
            part = pl.ds(start, tile)
            return ref.at[:, part] if lead is None else ref.at[lead, :, part]
        start -= width


def weight_copies(mid, tile, jobs, own_refs, got_refs, send, recv):
    me, my_far, _ = here(mid)
    copies = []
    for at, (bit, mask, chunk) in enumerate(jobs):
        block = flip(my_far, mask)
        source = chunk_at(chunk, tile, got_refs, block) if mask else chunk_at(
            chunk, tile, own_refs, None
        )
        copies.append(
            remote(
                source,
                chunk_at(chunk, tile, got_refs, block),
                send.at[at],
                recv.at[at],
                {"dp": join(me, flip(my_far, bit), mid)},
            )
        )
    return copies


class Halving:
    def __init__(self, bits, index, device, rows, out_ref, in_ref, acc_ref, own_ref, send, recv):
        self.bits, self.index, self.device, self.rows = bits, index, device, rows
        self.out_ref, self.in_ref, self.acc_ref, self.own_ref = out_ref, in_ref, acc_ref, own_ref
        self.send, self.recv = send, recv
        size = 1 << len(bits)
        self.stage_of = {
            mask: min(at for at, bit in enumerate(bits) if mask & bit) for mask in range(1, size)
        }
        later = [mask for mask in range(1, size) if self.stage_of[mask]]
        self.slot = {mask: at for at, mask in enumerate(later)}
        self.copies = []

    def masks(self, stage):
        return [mask for mask, at in self.stage_of.items() if at == stage]

    def start(self, stage):
        bit = self.bits[stage]
        for mask in self.masks(stage):
            copy = remote(
                self.out_ref.at[mask - 1],
                self.in_ref.at[mask - 1],
                self.send.at[mask - 1],
                self.recv.at[mask - 1],
                self.device(flip(self.index, bit)),
            )
            copy.start()
            self.copies.append((stage, copy))

    def receive(self, stage):
        for at, copy in self.copies:
            if at == stage:
                copy.wait_recv()
        rows, bit = self.rows, self.bits[stage]
        last = stage + 1 == len(self.bits)

        def add(at, carry):
            window = pl.ds(pl.multiple_of(at * rows, rows), rows)
            for mask in self.masks(stage):
                value = self.in_ref[mask - 1, window, :].astype(jnp.float32)
                rest = mask - bit
                if not rest:
                    self.own_ref[window, :] = self.own_ref[window, :] + value
                else:
                    value = self.acc_ref[self.slot[rest], window, :] + value
                    if self.stage_of[rest] == stage + 1:
                        self.out_ref[rest - 1, window, :] = value.astype(self.out_ref.dtype)
                    else:
                        self.acc_ref[self.slot[rest], window, :] = value
            return carry

        lax.fori_loop(0, self.own_ref.shape[0] // rows, add, 0)
        if not last:
            self.start(stage + 1)

    def finish(self):
        for _, copy in self.copies:
            copy.wait_send()


def front_kernel(mid, w_mid, tile, jobs, x_ref, gain_ref, bias_ref, pw_ref, wq_ref, wkv_ref, pwg_ref,
                 vg_ref, gq_ref, gkv_ref, normed, stat_out, stat_in, pw_send, pw_recv, st_send,
                 st_recv, far_send, far_recv, near_send, near_recv, twin_send, twin_recv, w_send,
                 w_recv):
    merge_count, tokens, part_width = x_ref.shape
    blocks, _, width = normed.shape
    far_count = vg_ref.shape[1]
    rows, wide = pwg_ref.shape[1:]
    feature = rows // merge_count
    tensor_count = lax.axis_size("tensor")
    me, my_far, tensor_index = here(mid)
    meet_all()
    pw_copies = []
    for step in range(1, NEAR):
        target = (me + step) % NEAR
        copy = remote(
            pw_ref.at[:, pl.ds(pl.multiple_of(target * wide, wide), wide)],
            pwg_ref.at[me],
            pw_send.at[step - 1],
            pw_recv.at[step - 1],
            {"dp": join(target, my_far, mid)},
        )
        copy.start()
        pw_copies.append(copy)
    w_copies = weight_copies(
        w_mid, tile, jobs, (wq_ref, wkv_ref), (gq_ref, gkv_ref), w_send, w_recv
    )
    early = 1
    for copy in w_copies[:early]:
        copy.start()

    count = merge_count * part_width
    total = jnp.zeros((tokens, 1), jnp.float32)
    for at in range(merge_count):
        total = total + jnp.sum(x_ref[at].astype(jnp.float32), axis=-1, keepdims=True)
    mean = total / count
    spread = jnp.zeros((tokens, 1), jnp.float32)
    for at in range(merge_count):
        centered = x_ref[at].astype(jnp.float32) - mean
        spread = spread + jnp.sum(centered * centered, axis=-1, keepdims=True)
    stat_out[0] = jnp.broadcast_to(mean, stat_out.shape[1:])
    stat_out[1] = jnp.broadcast_to(spread, stat_out.shape[1:])
    stat_copies = []
    for step in range(1, tensor_count):
        copy = remote(
            stat_out,
            stat_in.at[step - 1],
            st_send.at[step - 1],
            st_recv.at[step - 1],
            {"tensor": (tensor_index + step) % tensor_count},
        )
        copy.start()
        stat_copies.append(copy)
    for copy in stat_copies:
        copy.wait_recv()
    means, spreads = [mean], [spread]
    for step in range(1, tensor_count):
        means.append(stat_in[step - 1, 0][:, :1])
        spreads.append(stat_in[step - 1, 1][:, :1])
    average = sum(means) / tensor_count
    variance = sum(s + count * (one - average) * (one - average) for s, one in zip(spreads, means))
    scale = lax.rsqrt(variance / (count * tensor_count) + vision_epsilon)
    merged = [
        (x_ref[at].astype(jnp.float32) - average) * scale * gain_ref[pl.ds(at, 1)]
        + bias_ref[pl.ds(at, 1)]
        for at in range(merge_count)
    ]
    far_copies = []
    for at in range(blocks):
        pieces = []
        for block in range(NEAR):
            start = join(block, at, mid) * feature
            pieces += [one[:, start : start + feature] for one in merged]
        normed[at] = jnp.concatenate(pieces, axis=1).astype(normed.dtype)
        goal = tensor_index * blocks + at
        mine = goal == my_far
        copy = remote(
            normed.at[at],
            vg_ref.at[me, my_far],
            far_send.at[at],
            far_recv.at[my_far],
            {"dp": join(me, goal, mid)},
        )
        pl.when(jnp.logical_not(mine))(copy.start)
        far_copies.append((mine, copy))

        @pl.when(mine)
        def _():
            vg_ref[me, my_far] = normed[at]

    for copy in w_copies[early:]:
        copy.start()
    holder = my_far // blocks == tensor_index

    def twin_copy(ahead, mask):
        block = flip(me, mask)
        return remote(
            vg_ref.at[block],
            vg_ref.at[block],
            twin_send.at[ahead - 1, mask],
            twin_recv.at[mask],
            {"tensor": (tensor_index + ahead) % tensor_count},
        )

    def near_copy(bit, mask):
        block = flip(me, mask)
        return remote(
            vg_ref.at[block],
            vg_ref.at[block],
            near_send.at[(bit | mask) - 1],
            near_recv.at[(bit | mask) - 1],
            {"dp": join(flip(me, bit), my_far, mid)},
        )

    @pl.when(holder)
    def _():
        for step in range(1, far_count):
            source = (my_far + step) % far_count
            remote(
                normed.at[0],
                vg_ref.at[me, source],
                far_send.at[0],
                far_recv.at[source],
                {"dp": join(me, source, mid)},
            ).wait_recv()
        near_copies = {mask | bit: near_copy(bit, mask) for bit, mask in ((2, 0), (1, 0), (1, 2))}
        twin_copies = []
        near_copies[2].start()
        near_copies[1].start()
        for mask in (0, 2, 1, 3):
            if mask:
                near_copies[mask].wait_recv()
            if mask == 2:
                near_copies[3].start()
            for ahead in range(1, tensor_count):
                copy = twin_copy(ahead, mask)
                copy.start()
                twin_copies.append(copy)
        for copy in list(near_copies.values()) + twin_copies:
            copy.wait_send()

    def keep(at, carry):
        window = pl.ds(pl.multiple_of(at * 16, 16), 16)
        pwg_ref[me, window] = pw_ref[window, pl.ds(pl.multiple_of(me * wide, wide), wide)]
        return carry

    lax.fori_loop(0, rows // 16, keep, 0)

    @pl.when(jnp.logical_not(holder))
    def _():
        for step in range(NEAR):
            twin_copy(1, step).wait_recv()

    for mine, copy in far_copies:
        pl.when(jnp.logical_not(mine))(copy.wait_send)
    for copy in stat_copies:
        copy.wait_send()
    for copy in pw_copies + w_copies:
        copy.wait()


def front(x, gain, bias, proj, w_query, w_kv, tile, jobs, data_count, tensor_count, mid, w_mid):
    merge_count, tokens, part_width = x.shape
    far_count = data_count // NEAR
    blocks = far_count // tensor_count
    width = merge_count * part_width // blocks
    rows, columns = proj.shape
    vmem = pl.BlockSpec(memory_space=pltpu.VMEM)
    anywhere = pl.BlockSpec(memory_space=pltpu.HBM)
    dma = pltpu.SemaphoreType.DMA
    return pl.pallas_call(
        functools.partial(front_kernel, mid, w_mid, tile, jobs),
        out_shape=(
            jax.ShapeDtypeStruct((NEAR, rows, columns // NEAR), proj.dtype),
            jax.ShapeDtypeStruct((NEAR, far_count, tokens, width), x.dtype),
            jax.ShapeDtypeStruct((far_count,) + w_query.shape, w_query.dtype),
            jax.ShapeDtypeStruct((far_count,) + w_kv.shape, w_kv.dtype),
        ),
        in_specs=[vmem] * 4 + [anywhere] * 2,
        out_specs=(vmem, vmem, anywhere, anywhere),
        scratch_shapes=[
            pltpu.VMEM((blocks, tokens, width), x.dtype),
            pltpu.VMEM((2, tokens, 128), jnp.float32),
            pltpu.VMEM((tensor_count - 1, 2, tokens, 128), jnp.float32),
            dma((NEAR - 1,)),
            dma((NEAR - 1,)),
            dma((tensor_count - 1,)),
            dma((tensor_count - 1,)),
            dma((blocks,)),
            dma((far_count,)),
            dma((NEAR - 1,)),
            dma((NEAR - 1,)),
            dma((tensor_count - 1, NEAR)),
            dma((NEAR,)),
            dma((len(jobs),)),
            dma((len(jobs),)),
        ],
        compiler_params=pltpu.CompilerParams(
            collective_id=0, has_side_effects=True, vmem_limit_bytes=40 << 20
        ),
        cost_estimate=pl.CostEstimate(flops=0, bytes_accessed=80 << 20, transcendentals=0),
    )(x, gain, bias, proj, w_query, w_kv)


def middle_kernel(mid, t_mid, tile, span, w_tile, jobs, vg_ref, pw_ref, pick_ref, rows_ref, spot_ref, text_ref,
                  gain_ref, wq_ref, wkv_ref, gq_in, gkv_in, a_ref, gq_ref, gkv_ref, own, acc, out,
                  held_ref, t_send, t_recv, tiles, got, r_send, r_recv, seq, sums, sums_in,
                  leaving, st_send, st_recv, near_send, near_recv, twin_send, twin_recv, w_send,
                  w_recv):
    near, far_count, tokens, width = vg_ref.shape
    _, seq_len, depth = a_ref.shape
    chunks = own.shape[0]
    data_index, data_count = lax.axis_index("dp"), lax.axis_size("dp")
    tensor_count = lax.axis_size("tensor")
    held = depth // tensor_count
    model_width = text_ref.shape[1] * tensor_count
    wide = got.shape[3]
    spots = spot_ref.shape[1]
    early = seq_len - span
    me, my_far, tensor_index = here(mid)
    t_me, t_far, _ = here(t_mid)
    shift = held // (far_count // tensor_count)
    bits = []
    while 1 << len(bits) < far_count:
        bits.append(1 << len(bits))
    meet_all()
    w_copies = weight_copies(
        mid, w_tile, jobs, (wq_ref, wkv_ref), (gq_ref, gkv_ref), w_send, w_recv
    )
    half = [copy for copy, job in zip(w_copies, jobs) if job[0] == far_count // 2]
    rest = [copy for copy, job in zip(w_copies, jobs) if job[0] != far_count // 2]
    for copy in half[:1]:
        copy.start()

    def compute(mask, chunk, dst_ref):
        term = jnp.dot(
            vg_ref[:, flip(t_far, mask)].reshape(near * tokens, width),
            pw_ref[:, pl.ds(chunk * tile, tile)],
            preferred_element_type=jnp.float32,
        )
        dst_ref[...] = term.astype(dst_ref.dtype)

    parts = []
    for chunk in range(chunks):
        one = Halving(
            bits, t_far, lambda far: {"dp": join(t_me, far, t_mid)}, 32, out.at[chunk],
            held_ref.at[chunk], acc.at[chunk], own.at[chunk], t_send.at[chunk], t_recv.at[chunk],
        )
        for mask in one.masks(0):
            compute(mask, chunk, out.at[chunk, mask - 1])
        one.start(0)
        parts.append(one)
    for copy in rest[:7]:
        copy.start()
    for chunk, one in enumerate(parts):
        for mask, slot in one.slot.items():
            compute(mask, chunk, acc.at[chunk, slot])
        compute(0, chunk, own.at[chunk])

    rows = math.gcd(early, span)

    def fill(start, image):
        window = pl.ds(pl.multiple_of(start, rows), rows)
        place = lax.broadcasted_iota(jnp.int32, (rows, seq_len), 1)
        chosen = jnp.where(place == rows_ref[window, :], 1.0, 0.0).astype(jnp.bfloat16)
        if image:
            slots = lax.broadcasted_iota(jnp.int32, (rows, spots), 0) + (start - early)
            drawn = jnp.where(slots == spot_ref[...], 1.0, 0.0)
            is_image = jnp.max(drawn, axis=-1, keepdims=True) > 0.5
            drawn = drawn.astype(jnp.bfloat16)
        squares = jnp.zeros((rows, 1), jnp.float32)
        for part in range(near):
            lanes = pl.ds(part * wide, wide)
            value = jnp.dot(chosen, text_ref[:, lanes], preferred_element_type=jnp.float32)
            if image:
                tokens_here = got[part].reshape(spots, wide)
                tile_rows = jnp.dot(drawn, tokens_here, preferred_element_type=jnp.float32)
                value = jnp.where(is_image, tile_rows, value)
            seq[window, lanes] = value.astype(seq.dtype)
            squares = squares + jnp.sum(value * value, axis=-1, keepdims=True)
        sums[window, :] = jnp.broadcast_to(squares, (rows, sums.shape[1]))

    def share(phase, low, count):
        window = pl.ds(low, count)
        copies = []
        for step in range(1, tensor_count):
            copy = remote(
                sums.at[window],
                sums_in.at[step - 1, window],
                st_send.at[phase, step - 1],
                st_recv.at[phase, step - 1],
                {"tensor": (tensor_index + step) % tensor_count},
            )
            copy.start()
            copies.append(copy)
        return copies

    def lanes_of(owner):
        return pl.ds(pl.multiple_of(owner * held, held), held)

    fine = math.gcd(rows, 32)

    def norm(target, low, count, store):
        def one(at, carry):
            window = pl.ds(pl.multiple_of(low + at * fine, fine), fine)
            squares = sums[window, :][:, :1]
            for step in range(1, tensor_count):
                squares = squares + sums_in[step - 1, window, :][:, :1]
            scale = lax.rsqrt(squares / model_width + decoder_epsilon)
            for part in range(held // shift):
                lanes = pl.ds(pl.multiple_of(join(target, part, mid) * shift, shift), shift)
                value = seq[window, lanes].astype(jnp.float32) * scale * gain_ref[:, lanes]
                store(window, part * shift, value.astype(jnp.bfloat16))
            return carry

        lax.fori_loop(0, count // fine, one, 0)

    def stay(window, start, value):
        lanes = pl.ds(pl.multiple_of(tensor_index * held + start, shift), shift)
        a_ref[me, window, lanes] = value

    def spread(phase, low, count):
        window = pl.ds(low, count)
        copies = []
        for step in range(1, NEAR):

            def leave(window, start, value):
                leaving[step - 1, window, pl.ds(start, shift)] = value

            norm(flip(me, step), low, count, leave)
            copy = remote(
                leaving.at[step - 1, window],
                a_ref.at[me, window, lanes_of(tensor_index)],
                near_send.at[phase, step - 1],
                near_recv.at[phase, step - 1],
                {"dp": join(flip(me, step), my_far, mid)},
            )
            copy.start()
            copies.append(copy)
        norm(me, low, count, stay)
        return copies

    def twin_copy(phase, low, count, ahead, step, owner):
        block, window = flip(me, step), pl.ds(low, count)
        return remote(
            a_ref.at[block, window, lanes_of(owner)],
            a_ref.at[block, window, lanes_of(owner)],
            twin_send.at[phase, ahead - 1, step],
            twin_recv.at[phase, ahead - 1, step],
            {"tensor": (tensor_index + ahead) % tensor_count},
        )

    def pass_on(phase, low, count, near_copies):
        copies = []
        for step in range(NEAR):
            if step:
                near_copies[step - 1].wait_recv()
            for ahead in range(1, tensor_count):
                copy = twin_copy(phase, low, count, ahead, step, tensor_index)
                copy.start()
                copies.append(copy)
        return copies

    def collect(phase, low, count):
        for ahead in range(1, tensor_count):
            for step in range(NEAR):
                owner = (tensor_index + tensor_count - ahead) % tensor_count
                twin_copy(phase, low, count, ahead, step, owner).wait_recv()

    for start in range(0, early, rows):
        fill(start, False)
    stat_copies = share(0, 0, early)
    for one in parts:
        one.receive(0)
    for copy in stat_copies:
        copy.wait_recv()
    near_early = spread(0, 0, early)
    for stage in range(1, len(bits)):
        for one in parts:
            one.receive(stage)

    place = lax.broadcasted_iota(jnp.int32, (pick_ref.shape[0], near * tokens), 1)
    chosen = jnp.where(place == pick_ref[...], 1.0, 0.0).astype(jnp.bfloat16)
    for chunk in range(chunks):
        image = own[chunk].astype(jnp.bfloat16)
        sorted_rows = jnp.dot(chosen, image, preferred_element_type=jnp.float32)
        tiles[:, :, pl.ds(chunk * tile, tile)] = sorted_rows.astype(tiles.dtype).reshape(
            tiles.shape[0], tiles.shape[1], tile
        )
    route_copies = []
    for step in range(1, data_count):
        target = (data_index + step) % data_count
        copy = remote(
            tiles.at[target],
            got.at[t_me, t_far],
            r_send.at[step - 1],
            r_recv.at[step - 1],
            {"dp": target},
        )
        copy.start()
        route_copies.append(copy)
    for copy in half[1:] + rest[7:]:
        copy.start()
    got[t_me, t_far] = tiles[data_index]
    twin_early = pass_on(0, 0, early, near_early)
    for copy in route_copies:
        copy.wait_recv()
    for start in range(early, seq_len, rows):
        fill(start, True)
    late_copies = share(1, early, span)
    for copy in late_copies:
        copy.wait_recv()
    near_late = spread(1, early, span)
    twin_late = pass_on(1, early, span, near_late)
    collect(0, 0, early)
    collect(1, early, span)
    for copy in near_early + near_late + twin_early + twin_late + stat_copies + late_copies:
        copy.wait_send()
    for copy in route_copies:
        copy.wait_send()
    for one in parts:
        one.finish()
    for copy in w_copies:
        copy.wait()


def middle_part(vg, pw, pick, rows, spots, span, text, gain, weights, gathered, w_tile, jobs, mid, t_mid):
    near, far_count, tokens, width = vg.shape
    columns = pw.shape[1]
    tensor_count = lax.axis_size("tensor")
    data_count = lax.axis_size("dp")
    tile = math.gcd(columns, 512)
    chunks = columns // tile
    seq_len, part_model = text.shape
    held = part_model // NEAR
    sent = pick.shape[0] // data_count
    vmem = pl.BlockSpec(memory_space=pltpu.VMEM)
    anywhere = pl.BlockSpec(memory_space=pltpu.HBM)
    dma = pltpu.SemaphoreType.DMA
    return pl.pallas_call(
        functools.partial(middle_kernel, mid, t_mid, tile, span, w_tile, jobs),
        out_shape=(jax.ShapeDtypeStruct((NEAR, seq_len, held * tensor_count), text.dtype),)
        + tuple(jax.ShapeDtypeStruct(one.shape, one.dtype) for one in gathered),
        in_specs=[vmem] * 7 + [anywhere] * 4,
        out_specs=(vmem, anywhere, anywhere),
        input_output_aliases={9: 1, 10: 2},
        scratch_shapes=[
            pltpu.VMEM((chunks, near * tokens, tile), jnp.float32),
            pltpu.VMEM((chunks, far_count // 2 - 1, near * tokens, tile), jnp.float32),
            pltpu.VMEM((chunks, far_count - 1, near * tokens, tile), vg.dtype),
            pltpu.VMEM((chunks, far_count - 1, near * tokens, tile), vg.dtype),
            dma((chunks, far_count - 1)),
            dma((chunks, far_count - 1)),
            pltpu.VMEM((data_count, sent, columns), vg.dtype),
            pltpu.VMEM((NEAR, far_count, sent, columns), vg.dtype),
            dma((data_count - 1,)),
            dma((data_count - 1,)),
            pltpu.VMEM((seq_len, part_model), text.dtype),
            pltpu.VMEM((seq_len, 128), jnp.float32),
            pltpu.VMEM((tensor_count - 1, seq_len, 128), jnp.float32),
            pltpu.VMEM((NEAR - 1, seq_len, held), text.dtype),
            dma((2, tensor_count - 1)),
            dma((2, tensor_count - 1)),
            dma((2, NEAR - 1)),
            dma((2, NEAR - 1)),
            dma((2, tensor_count - 1, NEAR)),
            dma((2, tensor_count - 1, NEAR)),
            dma((len(jobs),)),
            dma((len(jobs),)),
        ],
        compiler_params=pltpu.CompilerParams(
            collective_id=1, has_side_effects=True, vmem_limit_bytes=48 << 20
        ),
        cost_estimate=pl.CostEstimate(
            flops=2 * far_count * near * tokens * width * columns,
            bytes_accessed=100 << 20,
            transcendentals=0,
        ),
    )(vg, pw, pick, rows, spots, text, gain, *weights, *gathered)


def product_kernel(mid, tile, jobs, have, a_ref, wq_ref, wkv_ref, gq_ref, gkv_ref, o_ref, w, acc,
                   out, held, send, recv, w_send, w_recv, load_sem):
    _, seq_len, _ = a_ref.shape
    depth = wq_ref.shape[0]
    far_count = gq_ref.shape[0]
    me, my_far, _ = here(mid)
    chunks = len(have)
    own_refs, got_refs = (wq_ref, wkv_ref), (gq_ref, gkv_ref)

    def place(mask, chunk):
        rows = pl.ds(pl.multiple_of(flip(my_far, mask) * depth, depth), depth)
        return w.at[rows, pl.ds(chunk * tile, tile)]

    def local(mask, chunk):
        if mask:
            return chunk_at(chunk, tile, got_refs, flip(my_far, mask))
        return chunk_at(chunk, tile, own_refs, None)

    loads = {}
    for chunk in range(chunks):
        for mask in sorted(have[chunk]):
            loads[mask, chunk] = pltpu.make_async_copy(
                local(mask, chunk), place(mask, chunk), load_sem.at[chunk, mask]
            )
            loads[mask, chunk].start()

    meet(mid, twin=False)
    arriving, waiting = {}, {chunk: [] for chunk in range(chunks)}
    for at, (bit, mask, chunk) in enumerate(jobs):
        kept = mask in have[chunk]
        copy = remote(
            local(mask, chunk) if kept else place(mask, chunk),
            place(mask, chunk),
            w_send.at[at],
            w_recv.at[at],
            {"dp": join(me, flip(my_far, bit), mid)},
        )
        arriving[bit | mask, chunk] = copy
        if kept:
            copy.start()
        else:
            waiting[chunk].append((mask, copy))
    seen = set()

    def ensure(mask, chunk):
        if (mask, chunk) not in seen:
            seen.add((mask, chunk))
            if (mask, chunk) in loads:
                loads[mask, chunk].wait()
            else:
                arriving[mask, chunk].wait_recv()

    def forward(chunk):
        for mask, copy in waiting.pop(chunk, ()):
            ensure(mask, chunk)
            copy.start()

    sums = []
    third = chunks // 3

    def compute(chunk):
        forward(chunk)
        for mask in range(far_count):
            ensure(mask, chunk)
        part = pl.ds(chunk * tile, tile)
        bits = (2, 1) if chunk % 3 == 1 else (1, 2)
        one = Halving(
            bits, me, lambda near: {"dp": join(near, my_far, mid)}, math.gcd(seq_len, 32),
            out.at[chunk], held.at[chunk], acc.at[chunk], o_ref.at[:, part], send.at[chunk],
            recv.at[chunk],
        )

        def fill(mask, dst_ref):
            term = jnp.dot(
                a_ref[flip(me, mask)], w[:, part], preferred_element_type=jnp.float32
            )
            dst_ref[...] = term.astype(dst_ref.dtype)

        for mask in one.masks(0):
            fill(mask, out.at[chunk, mask - 1])
        one.start(0)
        for mask, slot in one.slot.items():
            fill(mask, acc.at[chunk, slot])
        fill(0, o_ref.at[:, part])
        sums.append(one)

    done = {0: 0, 1: 0}

    def reduce(stage, upto):
        for one in sums[done[stage] : upto]:
            one.receive(stage)
        done[stage] = max(done[stage], upto)

    for chunk in range(2 * third):
        compute(chunk)
    reduce(0, third)
    for chunk in range(2 * third, chunks):
        forward(chunk)
        reduce(0, 2 * third)
        if chunk > 2 * third:
            reduce(1, 2 * third)
        compute(chunk)
    reduce(0, chunks)
    reduce(1, chunks)
    for one in sums:
        one.finish()
    for copy in arriving.values():
        copy.wait_send()


def product_blocks(a, weights, gathered, tile, jobs, have, mid):
    _, seq_len, depth = a.shape
    columns = sum(one.shape[1] for one in weights)
    chunks = columns // tile
    vmem = pl.BlockSpec(memory_space=pltpu.VMEM)
    anywhere = pl.BlockSpec(memory_space=pltpu.HBM)
    far_count = gathered[0].shape[0]
    dma = pltpu.SemaphoreType.DMA
    return pl.pallas_call(
        functools.partial(product_kernel, mid, tile, jobs, have),
        out_shape=jax.ShapeDtypeStruct((seq_len, columns), jnp.float32),
        in_specs=[vmem] + [anywhere] * 4,
        out_specs=vmem,
        scratch_shapes=[
            pltpu.VMEM((depth, columns), jnp.bfloat16),
            pltpu.VMEM((chunks, NEAR // 2 - 1, seq_len, tile), jnp.float32),
            pltpu.VMEM((chunks, NEAR - 1, seq_len, tile), jnp.bfloat16),
            pltpu.VMEM((chunks, NEAR - 1, seq_len, tile), jnp.bfloat16),
            dma((chunks, NEAR - 1)),
            dma((chunks, NEAR - 1)),
            dma((len(jobs),)),
            dma((len(jobs),)),
            dma((chunks, far_count)),
        ],
        compiler_params=pltpu.CompilerParams(
            collective_id=2, has_side_effects=True, vmem_limit_bytes=56 << 20
        ),
        cost_estimate=pl.CostEstimate(
            flops=2 * NEAR * seq_len * depth * columns,
            bytes_accessed=200 << 20,
            transcendentals=0,
        ),
    )(a, *weights, *gathered)


def attend_kernel(group, q_ref, k_ref, v_ref, cos_ref, sin_ref, down_ref, across_ref, o_ref):
    cosine, sine = cos_ref[...], sin_ref[...]

    def turn(rows):
        return (rows * cosine + pltpu.roll(rows, HEAD_WIDTH // 2, 1) * sine).astype(jnp.bfloat16)

    key_rows = turn(k_ref[...])
    value_rows = v_ref[...].astype(jnp.bfloat16)
    seq_len = key_rows.shape[0]
    allowed = down_ref[...] >= across_ref[...]
    row_at = lax.broadcasted_iota(jnp.int32, (seq_len, seq_len), 0)
    home = jnp.where(row_at == across_ref[...], 1.0, 0.0).astype(jnp.bfloat16)
    contexts = []
    for head in range(group):
        part = pl.ds(head * HEAD_WIDTH, HEAD_WIDTH)
        query_rows = turn(q_ref[:, part])
        scores = lax.dot_general(
            query_rows, key_rows, (((1,), (1,)), ((), ())), preferred_element_type=jnp.float32
        ) * HEAD_WIDTH ** (-0.5)
        scores = jnp.where(allowed, scores, -1e30)
        exponentials = jnp.exp(scores - jnp.max(scores, axis=-1, keepdims=True))
        weights = exponentials / jnp.sum(exponentials, axis=-1, keepdims=True)
        context = jnp.dot(
            weights.astype(jnp.bfloat16), value_rows, preferred_element_type=jnp.float32
        )
        contexts.append(context.astype(jnp.bfloat16))
    ordered = jnp.dot(
        home, jnp.concatenate(contexts, axis=1), preferred_element_type=jnp.float32
    )
    o_ref[...] = ordered.astype(o_ref.dtype)


def attend(product, positions, part_query):
    seq_len, columns = product.shape
    group = QUERY_HEADS // KEY_VALUE_HEADS
    local_kv = part_query // HEAD_WIDTH // group
    key_at = part_query // HEAD_WIDTH
    half_width = HEAD_WIDTH // 2
    exponents = jnp.arange(half_width, dtype=jnp.float32) * (2.0 / HEAD_WIDTH)
    frequency = rope_base ** (-exponents)
    angles = positions.astype(jnp.float32)[:, None] * frequency[None, :]
    cosine, sine = jnp.cos(angles), jnp.sin(angles)
    cosine = jnp.concatenate([cosine, cosine], axis=1)
    sine = jnp.concatenate([-sine, sine], axis=1)
    table = pl.BlockSpec((seq_len, HEAD_WIDTH), lambda g: (0, 0))
    return pl.pallas_call(
        functools.partial(attend_kernel, group),
        grid=(local_kv,),
        out_shape=jax.ShapeDtypeStruct((seq_len, part_query), jnp.bfloat16),
        in_specs=[
            pl.BlockSpec((seq_len, group * HEAD_WIDTH), lambda g: (0, g)),
            pl.BlockSpec((seq_len, HEAD_WIDTH), lambda g: (0, key_at + g)),
            pl.BlockSpec((seq_len, HEAD_WIDTH), lambda g: (0, key_at + local_kv + g)),
            table,
            table,
            pl.BlockSpec((seq_len, 1), lambda g: (0, 0)),
            pl.BlockSpec((1, seq_len), lambda g: (0, 0)),
        ],
        out_specs=pl.BlockSpec((seq_len, group * HEAD_WIDTH), lambda g: (0, g)),
        compiler_params=pltpu.CompilerParams(vmem_limit_bytes=24 << 20),
    )(product, product, product, cosine, sine, positions[:, None], positions[None, :])


def per_device(
    vis_rows,
    ln_gain,
    ln_bias,
    proj_weight,
    text_rows,
    attn_gain,
    w_query,
    key_value_weight,
    tile_counts,
    image_offsets,
):
    data_count = lax.axis_size("dp")
    data_index = lax.axis_index("dp")
    tensor_count = lax.axis_size("tensor")
    tensor_index = lax.axis_index("tensor")
    tile_rows, tile_tok, merge_count, part_width = vis_rows.shape
    feature = proj_weight.shape[0]
    part_model = proj_weight.shape[2]
    tokens = tile_rows * tile_tok
    mid = middle_size(data_count, tensor_count)
    t_mid = 1
    far_count = data_count // NEAR
    depth = w_query.shape[0]
    weights = (w_query, key_value_weight.reshape(depth, -1))
    tile = math.gcd(256, *(one.shape[1] for one in weights))
    chunks = sum(one.shape[1] for one in weights) // tile
    plan, have = gather_plan(far_count, chunks)

    start = tensor_index * part_width
    gain = lax.dynamic_slice_in_dim(ln_gain, start, part_width, 1)
    bias = lax.dynamic_slice_in_dim(ln_bias, start, part_width, 1)
    rows_in = vis_rows.reshape(tokens, merge_count, part_width).transpose(1, 0, 2)
    proj = proj_weight.transpose(1, 0, 2).reshape(merge_count * feature, part_model)
    proj, normed, *gathered = front(
        rows_in, gain, bias, proj, *weights, tile, plan["front"], data_count, tensor_count,
        t_mid, mid,
    )

    max_tiles = 2 * tile_rows
    tile_ends = jnp.cumsum(tile_counts)
    tile_firsts = tile_ends - tile_counts
    far_index = far_of(data_index, t_mid)
    sources = join(jnp.arange(NEAR, dtype=jnp.int32), far_index, t_mid)
    ranks = (sources[None, :] - tile_firsts[:, None]) % data_count
    taken = jnp.clip((tile_firsts[:, None] + ranks) // data_count, 0, tile_rows - 1)
    taken = taken + jnp.arange(NEAR, dtype=jnp.int32)[None, :] * tile_rows
    token_at = jnp.arange(tile_tok, dtype=jnp.int32)
    pick = (taken.reshape(-1, 1) * tile_tok + token_at[None, :]).reshape(-1, 1)

    is_mine = jnp.arange(data_count, dtype=jnp.int32) == data_index
    my_first = jnp.sum(jnp.where(is_mine, tile_firsts, 0))
    my_count = jnp.sum(jnp.where(is_mine, tile_counts, 0))
    far_ids = jnp.arange(far_count, dtype=jnp.int32)[:, None]
    tile_ids = join(jnp.arange(NEAR, dtype=jnp.int32)[None, :], far_ids, t_mid).reshape(-1)
    order = (tile_ids - my_first) % data_count
    spots = order[:, None] * tile_tok + token_at[None, :]
    spots = jnp.where((order < my_count)[:, None], spots, -1).reshape(1, -1)

    seq_len = text_rows.shape[1]
    image_span = max_tiles * tile_tok
    offset = image_offsets[0]
    outside = jnp.arange(seq_len - image_span, dtype=jnp.int32)
    outside = jnp.where(outside < offset, outside, outside + image_span)
    positions = jnp.concatenate([outside, offset + jnp.arange(image_span, dtype=jnp.int32)])
    gain = lax.dynamic_slice_in_dim(attn_gain, tensor_index * part_model, part_model, 0)
    sequence, *gathered = middle_part(
        normed, proj.reshape(-1, proj.shape[2]), pick, positions[:, None], spots, image_span,
        text_rows[0], gain[None, :], weights, gathered, tile, plan["sequence"], mid,
        t_mid,
    )
    product = product_blocks(sequence, weights, gathered, tile, plan["product"], have, mid)
    context = attend(product, positions, w_query.shape[1])
    return context[None]


def solution(mesh):
    in_specs = (
        P(None, "dp", None, "tensor"),
        P(),
        P(),
        P("dp", None, "tensor"),
        P("dp", None, "tensor"),
        P(),
        P("dp", "tensor"),
        P("dp", None, "tensor"),
        P(),
        P("dp"),
    )
    out_specs = P("dp", None, "tensor")
    return jax.shard_map(
        per_device, mesh=mesh, in_specs=in_specs, out_specs=out_specs, check_vma=False
    )
```

```python
import functools
import math

import jax
import jax.numpy as jnp
from jax import lax
from jax.experimental import pallas as pl
from jax.experimental.pallas import tpu as pltpu
from jax.sharding import PartitionSpec as P

QUERY_HEADS = 32
KEY_VALUE_HEADS = 8
HEAD_WIDTH = 128


vision_epsilon = 1e-06
decoder_epsilon = 1e-05
rope_base = 500000.0

MESH = pl.DeviceIdType.MESH
NEAR = 4


def near_of(index, mid):
    return index // (2 * mid) % 2 * 2 + index % 2


def far_of(index, mid):
    return index // (4 * mid) * mid + index // 2 % mid


def join(near, far, mid):
    return (far // mid * 2 + near // 2) * (2 * mid) + far % mid * 2 + near % 2


def middle_size(data_count, tensor_count):
    spare = int(math.log2(data_count)) - int(math.log2(tensor_count)) - 1
    return 1 << (min(2, spare) - 1)


def here(mid):
    data_index = lax.axis_index("dp")
    return near_of(data_index, mid), far_of(data_index, mid), lax.axis_index("tensor")


def meet(mid, near=True, far=True, twin=True):
    me, my_far, tensor_index = here(mid)
    far_count = lax.axis_size("dp") // NEAR
    tensor_count = lax.axis_size("tensor")
    targets = []
    if near:
        targets += [{"dp": join((me + s) % NEAR, my_far, mid)} for s in range(1, NEAR)]
    if far:
        targets += [{"dp": join(me, (my_far + s) % far_count, mid)} for s in range(1, far_count)]
    if twin:
        targets += [{"tensor": (tensor_index + s) % tensor_count} for s in range(1, tensor_count)]
    barrier = pltpu.get_barrier_semaphore()
    for target in targets:
        pl.semaphore_signal(barrier, inc=1, device_id=target, device_id_type=MESH)
    pl.semaphore_wait(barrier, len(targets))


def meet_all():
    data_index, data_count = lax.axis_index("dp"), lax.axis_size("dp")
    tensor_index, tensor_count = lax.axis_index("tensor"), lax.axis_size("tensor")
    targets = [{"dp": (data_index + s) % data_count} for s in range(1, data_count)]
    targets += [{"tensor": (tensor_index + s) % tensor_count} for s in range(1, tensor_count)]
    barrier = pltpu.get_barrier_semaphore()
    for target in targets:
        pl.semaphore_signal(barrier, inc=1, device_id=target, device_id_type=MESH)
    pl.semaphore_wait(barrier, len(targets))


def remote(src_ref, dst_ref, send_sem, recv_sem, device):
    return pltpu.make_async_remote_copy(
        src_ref=src_ref,
        dst_ref=dst_ref,
        send_sem=send_sem,
        recv_sem=recv_sem,
        device_id=device,
        device_id_type=MESH,
    )


def flip(index, bits):
    bit = 1
    while bit <= bits:
        if bits & bit:
            index = index + bit - 2 * bit * (index // bit % 2)
        bit *= 2
    return index


def gather_items(far_count):
    items, masks, bit = [], [0], far_count // 2
    while bit:
        items += [(bit, mask) for mask in masks]
        masks = masks + [mask | bit for mask in masks]
        bit //= 2
    return items


def gather_plan(far_count, chunks):
    third = chunks // 3
    high = far_count // 2
    items = gather_items(far_count)
    plan = {"front": [], "sequence": [], "product": []}
    have = {chunk: {0} for chunk in range(chunks)}
    plan["front"] = [(high, 0, chunk) for chunk in range(third)]
    plan["sequence"] = [(high, 0, chunk) for chunk in range(third, 2 * third)]
    plan["sequence"] += [
        (bit, 0, chunk) for bit, mask in items if not mask and bit != high
        for chunk in range(chunks)
    ]
    plan["sequence"] += [
        (bit, mask, chunk) for bit, mask in items if mask == high for chunk in range(third)
    ]
    for bit, mask, chunk in plan["front"] + plan["sequence"]:
        have[chunk].add(bit | mask)
    done = plan["front"] + plan["sequence"]
    for chunk in range(chunks):
        plan["product"] += [
            (bit, mask, chunk) for bit, mask in items if (bit, mask, chunk) not in done
        ]
    return plan, have


def chunk_at(chunk, tile, refs, lead):
    start = chunk * tile
    for ref in refs:
        width = ref.shape[-1]
        if start < width:
            part = pl.ds(start, tile)
            return ref.at[:, part] if lead is None else ref.at[lead, :, part]
        start -= width


def weight_copies(mid, tile, jobs, own_refs, got_refs, send, recv):
    me, my_far, _ = here(mid)
    copies = []
    for at, (bit, mask, chunk) in enumerate(jobs):
        block = flip(my_far, mask)
        source = chunk_at(chunk, tile, got_refs, block) if mask else chunk_at(
            chunk, tile, own_refs, None
        )
        copies.append(
            remote(
                source,
                chunk_at(chunk, tile, got_refs, block),
                send.at[at],
                recv.at[at],
                {"dp": join(me, flip(my_far, bit), mid)},
            )
        )
    return copies


class Halving:
    def __init__(self, bits, index, device, rows, out_ref, in_ref, acc_ref, own_ref, send, recv):
        self.bits, self.index, self.device, self.rows = bits, index, device, rows
        self.out_ref, self.in_ref, self.acc_ref, self.own_ref = out_ref, in_ref, acc_ref, own_ref
        self.send, self.recv = send, recv
        size = 1 << len(bits)
        self.stage_of = {
            mask: min(at for at, bit in enumerate(bits) if mask & bit) for mask in range(1, size)
        }
        later = [mask for mask in range(1, size) if self.stage_of[mask]]
        self.slot = {mask: at for at, mask in enumerate(later)}
        self.copies = []

    def masks(self, stage):
        return [mask for mask, at in self.stage_of.items() if at == stage]

    def start(self, stage):
        bit = self.bits[stage]
        for mask in self.masks(stage):
            copy = remote(
                self.out_ref.at[mask - 1],
                self.in_ref.at[mask - 1],
                self.send.at[mask - 1],
                self.recv.at[mask - 1],
                self.device(flip(self.index, bit)),
            )
            copy.start()
            self.copies.append((stage, copy))

    def receive(self, stage):
        for at, copy in self.copies:
            if at == stage:
                copy.wait_recv()
        rows, bit = self.rows, self.bits[stage]
        last = stage + 1 == len(self.bits)

        def add(at, carry):
            window = pl.ds(pl.multiple_of(at * rows, rows), rows)
            for mask in self.masks(stage):
                value = self.in_ref[mask - 1, window, :].astype(jnp.float32)
                rest = mask - bit
                if not rest:
                    self.own_ref[window, :] = self.own_ref[window, :] + value
                else:
                    value = self.acc_ref[self.slot[rest], window, :] + value
                    if self.stage_of[rest] == stage + 1:
                        self.out_ref[rest - 1, window, :] = value.astype(self.out_ref.dtype)
                    else:
                        self.acc_ref[self.slot[rest], window, :] = value
            return carry

        lax.fori_loop(0, self.own_ref.shape[0] // rows, add, 0)
        if not last:
            self.start(stage + 1)

    def finish(self):
        for _, copy in self.copies:
            copy.wait_send()


def front_kernel(mid, w_mid, tile, jobs, x_ref, gain_ref, bias_ref, pw_ref, wq_ref, wkv_ref, pwg_ref,
                 vg_ref, gq_ref, gkv_ref, normed, stat_out, stat_in, pw_send, pw_recv, st_send,
                 st_recv, far_send, far_recv, near_send, near_recv, twin_send, twin_recv, w_send,
                 w_recv):
    merge_count, tokens, part_width = x_ref.shape
    blocks, _, width = normed.shape
    far_count = vg_ref.shape[1]
    rows, wide = pwg_ref.shape[1:]
    feature = rows // merge_count
    tensor_count = lax.axis_size("tensor")
    me, my_far, tensor_index = here(mid)
    meet_all()
    pw_copies = []
    for step in range(1, NEAR):
        target = (me + step) % NEAR
        copy = remote(
            pw_ref.at[:, pl.ds(pl.multiple_of(target * wide, wide), wide)],
            pwg_ref.at[me],
            pw_send.at[step - 1],
            pw_recv.at[step - 1],
            {"dp": join(target, my_far, mid)},
        )
        copy.start()
        pw_copies.append(copy)
    w_copies = weight_copies(
        w_mid, tile, jobs, (wq_ref, wkv_ref), (gq_ref, gkv_ref), w_send, w_recv
    )
    early = 1
    for copy in w_copies[:early]:
        copy.start()

    count = merge_count * part_width
    total = jnp.zeros((tokens, 1), jnp.float32)
    for at in range(merge_count):
        total = total + jnp.sum(x_ref[at].astype(jnp.float32), axis=-1, keepdims=True)
    mean = total / count
    spread = jnp.zeros((tokens, 1), jnp.float32)
    for at in range(merge_count):
        centered = x_ref[at].astype(jnp.float32) - mean
        spread = spread + jnp.sum(centered * centered, axis=-1, keepdims=True)
    stat_out[0] = jnp.broadcast_to(mean, stat_out.shape[1:])
    stat_out[1] = jnp.broadcast_to(spread, stat_out.shape[1:])
    stat_copies = []
    for step in range(1, tensor_count):
        copy = remote(
            stat_out,
            stat_in.at[step - 1],
            st_send.at[step - 1],
            st_recv.at[step - 1],
            {"tensor": (tensor_index + step) % tensor_count},
        )
        copy.start()
        stat_copies.append(copy)
    for copy in stat_copies:
        copy.wait_recv()
    means, spreads = [mean], [spread]
    for step in range(1, tensor_count):
        means.append(stat_in[step - 1, 0][:, :1])
        spreads.append(stat_in[step - 1, 1][:, :1])
    average = sum(means) / tensor_count
    variance = sum(s + count * (one - average) * (one - average) for s, one in zip(spreads, means))
    scale = lax.rsqrt(variance / (count * tensor_count) + vision_epsilon)
    merged = [
        (x_ref[at].astype(jnp.float32) - average) * scale * gain_ref[pl.ds(at, 1)]
        + bias_ref[pl.ds(at, 1)]
        for at in range(merge_count)
    ]
    far_copies = []
    for at in range(blocks):
        pieces = []
        for block in range(NEAR):
            start = join(block, at, mid) * feature
            pieces += [one[:, start : start + feature] for one in merged]
        normed[at] = jnp.concatenate(pieces, axis=1).astype(normed.dtype)
        goal = tensor_index * blocks + at
        mine = goal == my_far
        copy = remote(
            normed.at[at],
            vg_ref.at[me, my_far],
            far_send.at[at],
            far_recv.at[my_far],
            {"dp": join(me, goal, mid)},
        )
        pl.when(jnp.logical_not(mine))(copy.start)
        far_copies.append((mine, copy))

        @pl.when(mine)
        def _():
            vg_ref[me, my_far] = normed[at]

    for copy in w_copies[early:]:
        copy.start()
    holder = my_far // blocks == tensor_index

    def twin_copy(ahead, mask):
        block = flip(me, mask)
        return remote(
            vg_ref.at[block],
            vg_ref.at[block],
            twin_send.at[ahead - 1, mask],
            twin_recv.at[mask],
            {"tensor": (tensor_index + ahead) % tensor_count},
        )

    def near_copy(bit, mask):
        block = flip(me, mask)
        return remote(
            vg_ref.at[block],
            vg_ref.at[block],
            near_send.at[(bit | mask) - 1],
            near_recv.at[(bit | mask) - 1],
            {"dp": join(flip(me, bit), my_far, mid)},
        )

    @pl.when(holder)
    def _():
        for step in range(1, far_count):
            source = (my_far + step) % far_count
            remote(
                normed.at[0],
                vg_ref.at[me, source],
                far_send.at[0],
                far_recv.at[source],
                {"dp": join(me, source, mid)},
            ).wait_recv()
        near_copies = {mask | bit: near_copy(bit, mask) for bit, mask in ((2, 0), (1, 0), (1, 2))}
        twin_copies = []
        near_copies[2].start()
        near_copies[1].start()
        for mask in (0, 2, 1, 3):
            if mask:
                near_copies[mask].wait_recv()
            if mask == 2:
                near_copies[3].start()
            for ahead in range(1, tensor_count):
                copy = twin_copy(ahead, mask)
                copy.start()
                twin_copies.append(copy)
        for copy in list(near_copies.values()) + twin_copies:
            copy.wait_send()

    def keep(at, carry):
        window = pl.ds(pl.multiple_of(at * 16, 16), 16)
        pwg_ref[me, window] = pw_ref[window, pl.ds(pl.multiple_of(me * wide, wide), wide)]
        return carry

    lax.fori_loop(0, rows // 16, keep, 0)

    @pl.when(jnp.logical_not(holder))
    def _():
        for step in range(NEAR):
            twin_copy(1, step).wait_recv()

    for mine, copy in far_copies:
        pl.when(jnp.logical_not(mine))(copy.wait_send)
    for copy in stat_copies:
        copy.wait_send()
    for copy in pw_copies + w_copies:
        copy.wait()


def front(x, gain, bias, proj, w_query, w_kv, tile, jobs, data_count, tensor_count, mid, w_mid):
    merge_count, tokens, part_width = x.shape
    far_count = data_count // NEAR
    blocks = far_count // tensor_count
    width = merge_count * part_width // blocks
    rows, columns = proj.shape
    vmem = pl.BlockSpec(memory_space=pltpu.VMEM)
    anywhere = pl.BlockSpec(memory_space=pltpu.HBM)
    dma = pltpu.SemaphoreType.DMA
    return pl.pallas_call(
        functools.partial(front_kernel, mid, w_mid, tile, jobs),
        out_shape=(
            jax.ShapeDtypeStruct((NEAR, rows, columns // NEAR), proj.dtype),
            jax.ShapeDtypeStruct((NEAR, far_count, tokens, width), x.dtype),
            jax.ShapeDtypeStruct((far_count,) + w_query.shape, w_query.dtype),
            jax.ShapeDtypeStruct((far_count,) + w_kv.shape, w_kv.dtype),
        ),
        in_specs=[vmem] * 4 + [anywhere] * 2,
        out_specs=(vmem, vmem, anywhere, anywhere),
        scratch_shapes=[
            pltpu.VMEM((blocks, tokens, width), x.dtype),
            pltpu.VMEM((2, tokens, 128), jnp.float32),
            pltpu.VMEM((tensor_count - 1, 2, tokens, 128), jnp.float32),
            dma((NEAR - 1,)),
            dma((NEAR - 1,)),
            dma((tensor_count - 1,)),
            dma((tensor_count - 1,)),
            dma((blocks,)),
            dma((far_count,)),
            dma((NEAR - 1,)),
            dma((NEAR - 1,)),
            dma((tensor_count - 1, NEAR)),
            dma((NEAR,)),
            dma((len(jobs),)),
            dma((len(jobs),)),
        ],
        compiler_params=pltpu.CompilerParams(
            collective_id=0, has_side_effects=True, vmem_limit_bytes=40 << 20
        ),
        cost_estimate=pl.CostEstimate(flops=0, bytes_accessed=80 << 20, transcendentals=0),
    )(x, gain, bias, proj, w_query, w_kv)


def middle_kernel(mid, t_mid, tile, span, w_tile, jobs, vg_ref, pw_ref, pick_ref, rows_ref, spot_ref, text_ref,
                  gain_ref, wq_ref, wkv_ref, gq_in, gkv_in, a_ref, gq_ref, gkv_ref, own, acc, out,
                  held_ref, t_send, t_recv, tiles, got, r_send, r_recv, seq, sums, sums_in,
                  leaving, st_send, st_recv, near_send, near_recv, twin_send, twin_recv, w_send,
                  w_recv):
    near, far_count, tokens, width = vg_ref.shape
    _, seq_len, depth = a_ref.shape
    chunks = own.shape[0]
    data_index, data_count = lax.axis_index("dp"), lax.axis_size("dp")
    tensor_count = lax.axis_size("tensor")
    held = depth // tensor_count
    model_width = text_ref.shape[1] * tensor_count
    wide = got.shape[3]
    spots = spot_ref.shape[1]
    early = seq_len - span
    me, my_far, tensor_index = here(mid)
    t_me, t_far, _ = here(t_mid)
    shift = held // (far_count // tensor_count)
    bits = []
    while 1 << len(bits) < far_count:
        bits.append(1 << len(bits))
    meet_all()
    w_copies = weight_copies(
        mid, w_tile, jobs, (wq_ref, wkv_ref), (gq_ref, gkv_ref), w_send, w_recv
    )
    half = [copy for copy, job in zip(w_copies, jobs) if job[0] == far_count // 2]
    rest = [copy for copy, job in zip(w_copies, jobs) if job[0] != far_count // 2]
    for copy in half[:1]:
        copy.start()

    def compute(mask, chunk, dst_ref):
        term = jnp.dot(
            vg_ref[:, flip(t_far, mask)].reshape(near * tokens, width),
            pw_ref[:, pl.ds(chunk * tile, tile)],
            preferred_element_type=jnp.float32,
        )
        dst_ref[...] = term.astype(dst_ref.dtype)

    parts = []
    for chunk in range(chunks):
        one = Halving(
            bits, t_far, lambda far: {"dp": join(t_me, far, t_mid)}, 32, out.at[chunk],
            held_ref.at[chunk], acc.at[chunk], own.at[chunk], t_send.at[chunk], t_recv.at[chunk],
        )
        for mask in one.masks(0):
            compute(mask, chunk, out.at[chunk, mask - 1])
        one.start(0)
        parts.append(one)
    for copy in rest[:7]:
        copy.start()
    for chunk, one in enumerate(parts):
        for mask, slot in one.slot.items():
            compute(mask, chunk, acc.at[chunk, slot])
        compute(0, chunk, own.at[chunk])

    rows = math.gcd(early, span)

    def fill(start, image):
        window = pl.ds(pl.multiple_of(start, rows), rows)
        place = lax.broadcasted_iota(jnp.int32, (rows, seq_len), 1)
        chosen = jnp.where(place == rows_ref[window, :], 1.0, 0.0).astype(jnp.bfloat16)
        if image:
            slots = lax.broadcasted_iota(jnp.int32, (rows, spots), 0) + (start - early)
            drawn = jnp.where(slots == spot_ref[...], 1.0, 0.0)
            is_image = jnp.max(drawn, axis=-1, keepdims=True) > 0.5
            drawn = drawn.astype(jnp.bfloat16)
        squares = jnp.zeros((rows, 1), jnp.float32)
        for part in range(near):
            lanes = pl.ds(part * wide, wide)
            value = jnp.dot(chosen, text_ref[:, lanes], preferred_element_type=jnp.float32)
            if image:
                tokens_here = got[part].reshape(spots, wide)
                tile_rows = jnp.dot(drawn, tokens_here, preferred_element_type=jnp.float32)
                value = jnp.where(is_image, tile_rows, value)
            seq[window, lanes] = value.astype(seq.dtype)
            squares = squares + jnp.sum(value * value, axis=-1, keepdims=True)
        sums[window, :] = jnp.broadcast_to(squares, (rows, sums.shape[1]))

    def share(phase, low, count):
        window = pl.ds(low, count)
        copies = []
        for step in range(1, tensor_count):
            copy = remote(
                sums.at[window],
                sums_in.at[step - 1, window],
                st_send.at[phase, step - 1],
                st_recv.at[phase, step - 1],
                {"tensor": (tensor_index + step) % tensor_count},
            )
            copy.start()
            copies.append(copy)
        return copies

    def lanes_of(owner):
        return pl.ds(pl.multiple_of(owner * held, held), held)

    fine = math.gcd(rows, 32)

    def norm(target, low, count, store):
        def one(at, carry):
            window = pl.ds(pl.multiple_of(low + at * fine, fine), fine)
            squares = sums[window, :][:, :1]
            for step in range(1, tensor_count):
                squares = squares + sums_in[step - 1, window, :][:, :1]
            scale = lax.rsqrt(squares / model_width + decoder_epsilon)
            for part in range(held // shift):
                lanes = pl.ds(pl.multiple_of(join(target, part, mid) * shift, shift), shift)
                value = seq[window, lanes].astype(jnp.float32) * scale * gain_ref[:, lanes]
                store(window, part * shift, value.astype(jnp.bfloat16))
            return carry

        lax.fori_loop(0, count // fine, one, 0)

    def stay(window, start, value):
        lanes = pl.ds(pl.multiple_of(tensor_index * held + start, shift), shift)
        a_ref[me, window, lanes] = value

    def spread(phase, low, count):
        window = pl.ds(low, count)
        copies = []
        for step in range(1, NEAR):

            def leave(window, start, value):
                leaving[step - 1, window, pl.ds(start, shift)] = value

            norm(flip(me, step), low, count, leave)
            copy = remote(
                leaving.at[step - 1, window],
                a_ref.at[me, window, lanes_of(tensor_index)],
                near_send.at[phase, step - 1],
                near_recv.at[phase, step - 1],
                {"dp": join(flip(me, step), my_far, mid)},
            )
            copy.start()
            copies.append(copy)
        norm(me, low, count, stay)
        return copies

    def twin_copy(phase, low, count, ahead, step, owner):
        block, window = flip(me, step), pl.ds(low, count)
        return remote(
            a_ref.at[block, window, lanes_of(owner)],
            a_ref.at[block, window, lanes_of(owner)],
            twin_send.at[phase, ahead - 1, step],
            twin_recv.at[phase, ahead - 1, step],
            {"tensor": (tensor_index + ahead) % tensor_count},
        )

    def pass_on(phase, low, count, near_copies):
        copies = []
        for step in range(NEAR):
            if step:
                near_copies[step - 1].wait_recv()
            for ahead in range(1, tensor_count):
                copy = twin_copy(phase, low, count, ahead, step, tensor_index)
                copy.start()
                copies.append(copy)
        return copies

    def collect(phase, low, count):
        for ahead in range(1, tensor_count):
            for step in range(NEAR):
                owner = (tensor_index + tensor_count - ahead) % tensor_count
                twin_copy(phase, low, count, ahead, step, owner).wait_recv()

    for start in range(0, early, rows):
        fill(start, False)
    stat_copies = share(0, 0, early)
    for one in parts:
        one.receive(0)
    for copy in stat_copies:
        copy.wait_recv()
    near_early = spread(0, 0, early)
    for stage in range(1, len(bits)):
        for one in parts:
            one.receive(stage)

    place = lax.broadcasted_iota(jnp.int32, (pick_ref.shape[0], near * tokens), 1)
    chosen = jnp.where(place == pick_ref[...], 1.0, 0.0).astype(jnp.bfloat16)
    for chunk in range(chunks):
        image = own[chunk].astype(jnp.bfloat16)
        sorted_rows = jnp.dot(chosen, image, preferred_element_type=jnp.float32)
        tiles[:, :, pl.ds(chunk * tile, tile)] = sorted_rows.astype(tiles.dtype).reshape(
            tiles.shape[0], tiles.shape[1], tile
        )
    route_copies = []
    for step in range(1, data_count):
        target = (data_index + step) % data_count
        copy = remote(
            tiles.at[target],
            got.at[t_me, t_far],
            r_send.at[step - 1],
            r_recv.at[step - 1],
            {"dp": target},
        )
        copy.start()
        route_copies.append(copy)
    for copy in half[1:] + rest[7:]:
        copy.start()
    got[t_me, t_far] = tiles[data_index]
    twin_early = pass_on(0, 0, early, near_early)
    for copy in route_copies:
        copy.wait_recv()
    for start in range(early, seq_len, rows):
        fill(start, True)
    late_copies = share(1, early, span)
    for copy in late_copies:
        copy.wait_recv()
    near_late = spread(1, early, span)
    twin_late = pass_on(1, early, span, near_late)
    collect(0, 0, early)
    collect(1, early, span)
    for copy in near_early + near_late + twin_early + twin_late + stat_copies + late_copies:
        copy.wait_send()
    for copy in route_copies:
        copy.wait_send()
    for one in parts:
        one.finish()
    for copy in w_copies:
        copy.wait()


def middle_part(vg, pw, pick, rows, spots, span, text, gain, weights, gathered, w_tile, jobs, mid, t_mid):
    near, far_count, tokens, width = vg.shape
    columns = pw.shape[1]
    tensor_count = lax.axis_size("tensor")
    data_count = lax.axis_size("dp")
    tile = math.gcd(columns, 512)
    chunks = columns // tile
    seq_len, part_model = text.shape
    held = part_model // NEAR
    sent = pick.shape[0] // data_count
    vmem = pl.BlockSpec(memory_space=pltpu.VMEM)
    anywhere = pl.BlockSpec(memory_space=pltpu.HBM)
    dma = pltpu.SemaphoreType.DMA
    return pl.pallas_call(
        functools.partial(middle_kernel, mid, t_mid, tile, span, w_tile, jobs),
        out_shape=(jax.ShapeDtypeStruct((NEAR, seq_len, held * tensor_count), text.dtype),)
        + tuple(jax.ShapeDtypeStruct(one.shape, one.dtype) for one in gathered),
        in_specs=[vmem] * 7 + [anywhere] * 4,
        out_specs=(vmem, anywhere, anywhere),
        input_output_aliases={9: 1, 10: 2},
        scratch_shapes=[
            pltpu.VMEM((chunks, near * tokens, tile), jnp.float32),
            pltpu.VMEM((chunks, far_count // 2 - 1, near * tokens, tile), jnp.float32),
            pltpu.VMEM((chunks, far_count - 1, near * tokens, tile), vg.dtype),
            pltpu.VMEM((chunks, far_count - 1, near * tokens, tile), vg.dtype),
            dma((chunks, far_count - 1)),
            dma((chunks, far_count - 1)),
            pltpu.VMEM((data_count, sent, columns), vg.dtype),
            pltpu.VMEM((NEAR, far_count, sent, columns), vg.dtype),
            dma((data_count - 1,)),
            dma((data_count - 1,)),
            pltpu.VMEM((seq_len, part_model), text.dtype),
            pltpu.VMEM((seq_len, 128), jnp.float32),
            pltpu.VMEM((tensor_count - 1, seq_len, 128), jnp.float32),
            pltpu.VMEM((NEAR - 1, seq_len, held), text.dtype),
            dma((2, tensor_count - 1)),
            dma((2, tensor_count - 1)),
            dma((2, NEAR - 1)),
            dma((2, NEAR - 1)),
            dma((2, tensor_count - 1, NEAR)),
            dma((2, tensor_count - 1, NEAR)),
            dma((len(jobs),)),
            dma((len(jobs),)),
        ],
        compiler_params=pltpu.CompilerParams(
            collective_id=1, has_side_effects=True, vmem_limit_bytes=48 << 20
        ),
        cost_estimate=pl.CostEstimate(
            flops=2 * far_count * near * tokens * width * columns,
            bytes_accessed=100 << 20,
            transcendentals=0,
        ),
    )(vg, pw, pick, rows, spots, text, gain, *weights, *gathered)


def product_kernel(mid, tile, jobs, have, a_ref, cos_ref, sin_ref, down_ref, across_ref, wq_ref,
                   wkv_ref, gq_ref, gkv_ref, y_ref, o_ref, keys, values, w, acc, out, held, send,
                   recv, w_send, w_recv, load_sem):
    _, seq_len, _ = a_ref.shape
    depth = wq_ref.shape[0]
    far_count = gq_ref.shape[0]
    me, my_far, _ = here(mid)
    chunks = len(have)
    own_refs, got_refs = (wq_ref, wkv_ref), (gq_ref, gkv_ref)

    def place(mask, chunk):
        rows = pl.ds(pl.multiple_of(flip(my_far, mask) * depth, depth), depth)
        return w.at[rows, pl.ds(chunk * tile, tile)]

    def local(mask, chunk):
        if mask:
            return chunk_at(chunk, tile, got_refs, flip(my_far, mask))
        return chunk_at(chunk, tile, own_refs, None)

    loads = {}
    for chunk in range(chunks):
        for mask in sorted(have[chunk]):
            loads[mask, chunk] = pltpu.make_async_copy(
                local(mask, chunk), place(mask, chunk), load_sem.at[chunk, mask]
            )
            loads[mask, chunk].start()

    meet(mid, twin=False)
    arriving, waiting = {}, {chunk: [] for chunk in range(chunks)}
    for at, (bit, mask, chunk) in enumerate(jobs):
        kept = mask in have[chunk]
        copy = remote(
            local(mask, chunk) if kept else place(mask, chunk),
            place(mask, chunk),
            w_send.at[at],
            w_recv.at[at],
            {"dp": join(me, flip(my_far, bit), mid)},
        )
        arriving[bit | mask, chunk] = copy
        if kept:
            copy.start()
        else:
            waiting[chunk].append((mask, copy))
    seen = set()

    def ensure(mask, chunk):
        if (mask, chunk) not in seen:
            seen.add((mask, chunk))
            if (mask, chunk) in loads:
                loads[mask, chunk].wait()
            else:
                arriving[mask, chunk].wait_recv()

    def forward(chunk):
        for mask, copy in waiting.pop(chunk, ()):
            ensure(mask, chunk)
            copy.start()

    sums = []
    third = chunks // 3

    def compute(chunk):
        forward(chunk)
        for mask in range(far_count):
            ensure(mask, chunk)
        part = pl.ds(chunk * tile, tile)
        bits = (2, 1) if chunk % 3 == 1 else (1, 2)
        one = Halving(
            bits, me, lambda near: {"dp": join(near, my_far, mid)}, math.gcd(seq_len, 32),
            out.at[chunk], held.at[chunk], acc.at[chunk], o_ref.at[:, part], send.at[chunk],
            recv.at[chunk],
        )

        def fill(mask, dst_ref):
            term = jnp.dot(
                a_ref[flip(me, mask)], w[:, part], preferred_element_type=jnp.float32
            )
            dst_ref[...] = term.astype(dst_ref.dtype)

        for mask in one.masks(0):
            fill(mask, out.at[chunk, mask - 1])
        one.start(0)
        for mask, slot in one.slot.items():
            fill(mask, acc.at[chunk, slot])
        fill(0, o_ref.at[:, part])
        sums.append(one)

    done = {0: 0, 1: 0}

    def reduce(stage, upto):
        for one in sums[done[stage] : upto]:
            one.receive(stage)
        done[stage] = max(done[stage], upto)

    group = QUERY_HEADS // KEY_VALUE_HEADS
    kv_width = keys.shape[1]
    kv_chunks = -(-2 * kv_width // tile)
    chunk_heads = tile // HEAD_WIDTH
    head_count = y_ref.shape[1] // HEAD_WIDTH

    def turn(value):
        rolled = pltpu.roll(value, HEAD_WIDTH // 2, 1)
        return (value * cos_ref[...] + rolled * sin_ref[...]).astype(jnp.bfloat16)

    def attend(low, high):
        def one_head(head, carry):
            source = pl.multiple_of(2 * kv_width + head * HEAD_WIDTH, HEAD_WIDTH)
            goal = pl.ds(pl.multiple_of(head * HEAD_WIDTH, HEAD_WIDTH), HEAD_WIDTH)
            lanes = pl.ds(pl.multiple_of(head // group * HEAD_WIDTH, HEAD_WIDTH), HEAD_WIDTH)
            scores = lax.dot_general(
                turn(o_ref[:, pl.ds(source, HEAD_WIDTH)]), keys[:, lanes],
                (((1,), (1,)), ((), ())), preferred_element_type=jnp.float32,
            ) * HEAD_WIDTH ** (-0.5)
            scores = jnp.where(down_ref[...] >= across_ref[...], scores, -1e30)
            exponentials = jnp.exp(scores - jnp.max(scores, axis=-1, keepdims=True))
            weights = exponentials / jnp.sum(exponentials, axis=-1, keepdims=True)
            context = jnp.dot(
                weights.astype(jnp.bfloat16), values[:, lanes], preferred_element_type=jnp.float32
            )
            row_at = lax.broadcasted_iota(jnp.int32, (seq_len, seq_len), 0)
            home = jnp.where(row_at == across_ref[...], 1.0, 0.0).astype(jnp.bfloat16)
            ordered = jnp.dot(
                home, context.astype(jnp.bfloat16), preferred_element_type=jnp.float32
            )
            y_ref[:, goal] = ordered.astype(y_ref.dtype)
            return carry

        if low < high:
            lax.fori_loop(low, high, one_head, 0)

    def heads_in(upto):
        return min(head_count, max(0, upto - kv_chunks) * chunk_heads)

    for chunk in range(2 * third):
        compute(chunk)
    reduce(0, third)
    for chunk in range(2 * third, chunks):
        forward(chunk)
        reduce(0, 2 * third)
        if chunk > 2 * third:
            reduce(1, 2 * third)
        compute(chunk)
    reduce(1, 2 * third)
    for lanes in range(0, kv_width, HEAD_WIDTH):
        part = pl.ds(lanes, HEAD_WIDTH)
        keys[:, part] = turn(o_ref[:, part])
    values[...] = o_ref[:, pl.ds(kv_width, kv_width)].astype(values.dtype)
    ready = heads_in(2 * third)
    reduce(0, chunks - 2)
    attend(0, ready // 2)
    reduce(0, chunks - 1)
    attend(ready // 2, ready)
    reduce(0, chunks)
    reduce(1, chunks - 2)
    attend(ready, heads_in(chunks - 2))
    reduce(1, chunks)
    attend(max(ready, heads_in(chunks - 2)), head_count)
    for one in sums:
        one.finish()
    for copy in arriving.values():
        copy.wait_send()


def product_blocks(a, positions, weights, gathered, tile, jobs, have, mid):
    _, seq_len, depth = a.shape
    columns = sum(one.shape[1] for one in weights)
    chunks = columns // tile
    vmem = pl.BlockSpec(memory_space=pltpu.VMEM)
    anywhere = pl.BlockSpec(memory_space=pltpu.HBM)
    far_count = gathered[0].shape[0]
    dma = pltpu.SemaphoreType.DMA
    kv_width = weights[0].shape[1] // 2
    half_width = HEAD_WIDTH // 2
    exponents = jnp.arange(half_width, dtype=jnp.float32) * (2.0 / HEAD_WIDTH)
    frequency = rope_base ** (-exponents)
    angles = positions.astype(jnp.float32)[:, None] * frequency[None, :]
    cosine, sine = jnp.cos(angles), jnp.sin(angles)
    cosine = jnp.concatenate([cosine, cosine], axis=1)
    sine = jnp.concatenate([-sine, sine], axis=1)
    return pl.pallas_call(
        functools.partial(product_kernel, mid, tile, jobs, have),
        out_shape=jax.ShapeDtypeStruct((seq_len, weights[1].shape[1]), jnp.bfloat16),
        in_specs=[vmem] * 5 + [anywhere] * 4,
        out_specs=vmem,
        scratch_shapes=[
            pltpu.VMEM((seq_len, columns), jnp.float32),
            pltpu.VMEM((seq_len, kv_width), jnp.bfloat16),
            pltpu.VMEM((seq_len, kv_width), jnp.bfloat16),
            pltpu.VMEM((depth, columns), jnp.bfloat16),
            pltpu.VMEM((chunks, NEAR // 2 - 1, seq_len, tile), jnp.float32),
            pltpu.VMEM((chunks, NEAR - 1, seq_len, tile), jnp.bfloat16),
            pltpu.VMEM((chunks, NEAR - 1, seq_len, tile), jnp.bfloat16),
            dma((chunks, NEAR - 1)),
            dma((chunks, NEAR - 1)),
            dma((len(jobs),)),
            dma((len(jobs),)),
            dma((chunks, far_count)),
        ],
        compiler_params=pltpu.CompilerParams(
            collective_id=2, has_side_effects=True, vmem_limit_bytes=56 << 20
        ),
        cost_estimate=pl.CostEstimate(
            flops=2 * NEAR * seq_len * depth * columns,
            bytes_accessed=200 << 20,
            transcendentals=0,
        ),
    )(a, cosine, sine, positions[:, None], positions[None, :], *weights, *gathered)


def per_device(
    vis_rows,
    ln_gain,
    ln_bias,
    proj_weight,
    text_rows,
    attn_gain,
    w_query,
    key_value_weight,
    tile_counts,
    image_offsets,
):
    data_count = lax.axis_size("dp")
    data_index = lax.axis_index("dp")
    tensor_count = lax.axis_size("tensor")
    tensor_index = lax.axis_index("tensor")
    tile_rows, tile_tok, merge_count, part_width = vis_rows.shape
    feature = proj_weight.shape[0]
    part_model = proj_weight.shape[2]
    tokens = tile_rows * tile_tok
    mid = middle_size(data_count, tensor_count)
    t_mid = 1
    far_count = data_count // NEAR
    depth = w_query.shape[0]
    weights = (key_value_weight.reshape(depth, -1), w_query)
    tile = math.gcd(256, *(one.shape[1] for one in weights))
    chunks = sum(one.shape[1] for one in weights) // tile
    plan, have = gather_plan(far_count, chunks)

    start = tensor_index * part_width
    gain = lax.dynamic_slice_in_dim(ln_gain, start, part_width, 1)
    bias = lax.dynamic_slice_in_dim(ln_bias, start, part_width, 1)
    rows_in = vis_rows.reshape(tokens, merge_count, part_width).transpose(1, 0, 2)
    proj = proj_weight.transpose(1, 0, 2).reshape(merge_count * feature, part_model)
    proj, normed, *gathered = front(
        rows_in, gain, bias, proj, *weights, tile, plan["front"], data_count, tensor_count,
        t_mid, mid,
    )

    max_tiles = 2 * tile_rows
    tile_ends = jnp.cumsum(tile_counts)
    tile_firsts = tile_ends - tile_counts
    far_index = far_of(data_index, t_mid)
    sources = join(jnp.arange(NEAR, dtype=jnp.int32), far_index, t_mid)
    ranks = (sources[None, :] - tile_firsts[:, None]) % data_count
    taken = jnp.clip((tile_firsts[:, None] + ranks) // data_count, 0, tile_rows - 1)
    taken = taken + jnp.arange(NEAR, dtype=jnp.int32)[None, :] * tile_rows
    token_at = jnp.arange(tile_tok, dtype=jnp.int32)
    pick = (taken.reshape(-1, 1) * tile_tok + token_at[None, :]).reshape(-1, 1)

    is_mine = jnp.arange(data_count, dtype=jnp.int32) == data_index
    my_first = jnp.sum(jnp.where(is_mine, tile_firsts, 0))
    my_count = jnp.sum(jnp.where(is_mine, tile_counts, 0))
    far_ids = jnp.arange(far_count, dtype=jnp.int32)[:, None]
    tile_ids = join(jnp.arange(NEAR, dtype=jnp.int32)[None, :], far_ids, t_mid).reshape(-1)
    order = (tile_ids - my_first) % data_count
    spots = order[:, None] * tile_tok + token_at[None, :]
    spots = jnp.where((order < my_count)[:, None], spots, -1).reshape(1, -1)

    seq_len = text_rows.shape[1]
    image_span = max_tiles * tile_tok
    offset = image_offsets[0]
    outside = jnp.arange(seq_len - image_span, dtype=jnp.int32)
    outside = jnp.where(outside < offset, outside, outside + image_span)
    positions = jnp.concatenate([outside, offset + jnp.arange(image_span, dtype=jnp.int32)])
    gain = lax.dynamic_slice_in_dim(attn_gain, tensor_index * part_model, part_model, 0)
    sequence, *gathered = middle_part(
        normed, proj.reshape(-1, proj.shape[2]), pick, positions[:, None], spots, image_span,
        text_rows[0], gain[None, :], weights, gathered, tile, plan["sequence"], mid,
        t_mid,
    )
    context = product_blocks(
        sequence, positions, weights, gathered, tile, plan["product"], have, mid
    )
    return context[None]


def solution(mesh):
    in_specs = (
        P(None, "dp", None, "tensor"),
        P(),
        P(),
        P("dp", None, "tensor"),
        P("dp", None, "tensor"),
        P(),
        P("dp", "tensor"),
        P("dp", None, "tensor"),
        P(),
        P("dp"),
    )
    out_specs = P("dp", None, "tensor")
    return jax.shard_map(
        per_device, mesh=mesh, in_specs=in_specs, out_specs=out_specs, check_vma=False
    )
```
